8 devices in a mesh: dp: 4 (over z, y, x), tp: 2 (over core).
Axes of the slice: x: 2, y: 2, z: 1, core: 2. Of those that a mesh axis runs over, the one named last changes fastest.
Arguments:
- node_lat: bfloat16 [64, 42, 512], P('dp', None, 'tp')
- edge_lat: bfloat16 [64, 300, 512], P('dp', None, 'tp')
- senders: int32 [300], replicated
- receivers: int32 [300], replicated
- grad_node: bfloat16 [64, 42, 512], P('dp', None, 'tp')
- grad_edge: bfloat16 [64, 300, 512], P('dp', None, 'tp')
- edge_w1: bfloat16 [2, 3, 512, 512], P(None, None, 'tp')
- edge_b1: float32 [2, 512], replicated
- edge_w2: bfloat16 [2, 512, 512], P(None, None, 'tp')
- edge_vec: float32 [2, 3, 512], P(None, None, 'tp')
- node_w1: bfloat16 [2, 2, 512, 512], P(None, None, 'tp')
- node_b1: float32 [2, 512], replicated
- node_w2: bfloat16 [2, 512, 512], P(None, None, 'tp')
- node_vec: float32 [2, 3, 512], P(None, None, 'tp')
Outputs:
- output 1: bfloat16 [64, 42, 512], P('dp', None, 'tp')
- output 2: bfloat16 [64, 300, 512], P('dp', None, 'tp')
- output 3: bfloat16 [64, 42, 512], P('dp', None, 'tp')
- output 4: bfloat16 [64, 300, 512], P('dp', None, 'tp')
- output 5: float32 [2, 3, 512, 512], P(None, None, 'tp')
- output 6: float32 [2, 512], replicated
- output 7: float32 [2, 512, 512], P(None, None, 'tp')
- output 8: float32 [2, 3, 512], P(None, None, 'tp')
- output 9: float32 [2, 2, 512, 512], P(None, None, 'tp')
- output 10: float32 [2, 512], replicated
- output 11: float32 [2, 512, 512], P(None, None, 'tp')
- output 12: float32 [2, 3, 512], P(None, None, 'tp')
All inputs are finite; a program needn't handle non-finite values.
Results may differ from the reference program's by a relative error of at most 0.02.
Values sent between devices are 32-bit elements.
A program may use at most 1 GiB of HBM per device.

```python
import jax
import jax.numpy as jnp
from jax import lax

D = 512
NODES = 42
EDGES = 300
BATCH = 64
LAYERS = 2
LN_EPS = 1e-5


def normal_draw(base_key, arr_shape):
    return jax.random.normal(base_key, arr_shape, jnp.float32)


def vec_draw(base_key):
    noise_val = normal_draw(base_key, (LAYERS, 3, D))
    scales = jnp.array([0.5, 0.3, 0.3], jnp.float32)[None, :, None]
    shifts = jnp.array([0.0, 1.0, 0.0], jnp.float32)[None, :, None]
    return noise_val * scales + shifts


def index_draw(base_key):
    idx_keys = jax.random.split(base_key, 4)
    extra_edges = EDGES - NODES
    senders = jnp.concatenate([
        jax.random.randint(idx_keys[0], (extra_edges,), 0, NODES, dtype=jnp.int32),
        jax.random.permutation(idx_keys[1], NODES).astype(jnp.int32)])
    receivers = jnp.concatenate([
        jax.random.permutation(idx_keys[2], NODES).astype(jnp.int32),
        jax.random.randint(idx_keys[3], (extra_edges,), 0, NODES, dtype=jnp.int32)])
    return senders, receivers


def setup_inputs(seed: int = 0) -> dict:
    sub_keys = jax.random.split(jax.random.key(seed), 13)
    senders, receivers = index_draw(sub_keys[12])
    node_shape = (BATCH, NODES, D)
    edge_shape = (BATCH, EDGES, D)
    return {
        'node_lat': normal_draw(sub_keys[0], node_shape).astype(jnp.bfloat16),
        'edge_lat': normal_draw(sub_keys[1], edge_shape).astype(jnp.bfloat16),
        'senders': senders,
        'receivers': receivers,
        'grad_node': normal_draw(sub_keys[2], node_shape).astype(jnp.bfloat16),
        'grad_edge': normal_draw(sub_keys[3], edge_shape).astype(jnp.bfloat16),
        'edge_w1': (normal_draw(sub_keys[4], (LAYERS, 3, D, D)) * (3 * D) ** -0.5).astype(jnp.bfloat16),
        'edge_b1': 0.5 * normal_draw(sub_keys[5], (LAYERS, D)),
        'edge_w2': (normal_draw(sub_keys[6], (LAYERS, D, D)) * D ** -0.5).astype(jnp.bfloat16),
        'edge_vec': vec_draw(sub_keys[7]),
        'node_w1': (normal_draw(sub_keys[8], (LAYERS, 2, D, D)) * (2 * D) ** -0.5).astype(jnp.bfloat16),
        'node_b1': 0.5 * normal_draw(sub_keys[9], (LAYERS, D)),
        'node_w2': (normal_draw(sub_keys[10], (LAYERS, D, D)) * D ** -0.5).astype(jnp.bfloat16),
        'node_vec': vec_draw(sub_keys[11]),
    }


def mlp_norm(inputs, w_first, b_first, w_second, norm_vec):
    hidden = b_first
    for block_id in range(len(inputs)):
        hidden = hidden + jnp.dot(inputs[block_id], w_first[block_id].astype(jnp.bfloat16), preferred_element_type=jnp.float32)
    act_bf = jax.nn.silu(hidden).astype(jnp.bfloat16)
    out_f32 = jnp.dot(act_bf, w_second.astype(jnp.bfloat16), preferred_element_type=jnp.float32) + norm_vec[0]
    row_mean = jnp.mean(out_f32, axis=-1, keepdims=True)
    centered = out_f32 - row_mean
    row_var = jnp.mean(centered * centered, axis=-1, keepdims=True)
    return (centered * lax.rsqrt(row_var + LN_EPS) * norm_vec[1] + norm_vec[2]).astype(jnp.bfloat16)


def layer_step(node_lat, edge_lat, senders, receivers, layer_par):
    edge_w1, edge_b1, edge_w2, edge_vec, node_w1, node_b1, node_w2, node_vec = layer_par
    send_lat = jnp.take(node_lat, senders, axis=0)
    recv_lat = jnp.take(node_lat, receivers, axis=0)
    edge_msg = mlp_norm((edge_lat, send_lat, recv_lat), edge_w1, edge_b1, edge_w2, edge_vec)
    node_agg = jax.ops.segment_sum(edge_msg.astype(jnp.float32), receivers, num_segments=node_lat.shape[0]).astype(jnp.bfloat16)
    node_msg = mlp_norm((node_lat, node_agg), node_w1, node_b1, node_w2, node_vec)
    new_node = (node_lat.astype(jnp.float32) + node_msg.astype(jnp.float32)).astype(jnp.bfloat16)
    new_edge = (edge_lat.astype(jnp.float32) + edge_msg.astype(jnp.float32)).astype(jnp.bfloat16)
    return new_node, new_edge


def sample_forward(node_lat, edge_lat, senders, receivers, params):
    def layer_body(carry_lat, layer_par):
        return layer_step(carry_lat[0], carry_lat[1], senders, receivers, layer_par), None
    final_lat, unused_out = lax.scan(layer_body, (node_lat, edge_lat), params)
    return final_lat


def reference(node_lat, edge_lat, senders, receivers, grad_node, grad_edge, edge_w1, edge_b1, edge_w2, edge_vec, node_w1, node_b1, node_w2, node_vec):
    params = (edge_w1.astype(jnp.float32), edge_b1, edge_w2.astype(jnp.float32), edge_vec,
              node_w1.astype(jnp.float32), node_b1, node_w2.astype(jnp.float32), node_vec)

    def forward_fn(node_one, edge_one, par_f32):
        return sample_forward(node_one, edge_one, senders, receivers, par_f32)

    def per_sample(grad_acc, sample):
        node_one, edge_one, gnode_one, gedge_one = sample
        fwd_outs, pullback = jax.vjp(forward_fn, node_one, edge_one, params)
        d_node, d_edge, d_params = pullback((gnode_one, gedge_one))
        grad_acc = tuple(acc_part + new_part for acc_part, new_part in zip(grad_acc, d_params))
        return grad_acc, (fwd_outs[0], fwd_outs[1], d_node, d_edge)

    zero_acc = tuple(jnp.zeros(par_arr.shape, jnp.float32) for par_arr in params)
    grad_acc, per_out = lax.scan(per_sample, zero_acc, (node_lat, edge_lat, grad_node, grad_edge))
    return (per_out[0], per_out[1], per_out[2], per_out[3],
            grad_acc[0], grad_acc[1], grad_acc[2], grad_acc[3],
            grad_acc[4], grad_acc[5], grad_acc[6], grad_acc[7])
```

```python
import functools

import jax
import jax.numpy as jnp
from jax import lax
from jax.experimental import pallas as pl
from jax.experimental.pallas import tpu as pltpu
from jax.sharding import PartitionSpec as P

BF = jnp.bfloat16
F32 = jnp.float32
MESH = pl.DeviceIdType.MESH
LN_EPS = 1e-5
NS = 8
NN = 42
NP = 48
NE = 300
D = 512
H = 256
ROWS = NS * NP


def dot(lhs, rhs, lc=1, rc=0):
    return lax.dot_general(lhs, rhs, (((lc,), (rc,)), ((), ())), preferred_element_type=F32)


def split3(x):
    hi = x.astype(BF)
    rest = x - hi.astype(F32)
    mid = rest.astype(BF)
    low = (rest - mid.astype(F32)).astype(BF)
    return hi, mid, low


def cat(lhs, rhs):
    return jnp.concatenate([lhs, rhs], axis=1)


def mean_cols(x):
    return jnp.sum(x, axis=1, keepdims=True) * (1.0 / D)


def sum_rows(x):
    return jnp.sum(x, axis=0, keepdims=True)


def norm_parts(centered):
    inv_std = lax.rsqrt(mean_cols(centered * centered) + LN_EPS)
    return centered * inv_std, inv_std


J_NW2, J_NW1, J_EW2, J_EW1 = 0, 1, 3, 4


def body(nl, el, gn, ge, w1e, w2e, w1n, w2n, b1e, b1n, vece, vecn, snd, rcv,
         o_n, o_e, o_dn, o_de, o_g, o_sm, spill,
         W1E, W2E, W1N, W2N, VE, VN, S3, R3, TT,
         E0, E1, E2, DE, HS, CS, R2, G, PS, PR,
         NST, NF, VF, SF, HN, CN, DN, DV, GS, GR, SM,
         lsem, ssem, rsem, csem, spsem):
    dp = lax.axis_index('dp')
    tp = lax.axis_index('tp')
    ot = 1 - tp
    partner = (dp, ot)

    def rdma(src, dst, idx):
        return pltpu.make_async_remote_copy(
            src_ref=src, dst_ref=dst, send_sem=ssem.at[idx], recv_sem=rsem.at[idx],
            device_id=partner, device_id_type=MESH)

    mine = pl.ds(tp * NS, NS)
    theirs = pl.ds(ot * NS, NS)
    loads = [
        (nl.at[mine], NST.at[0]), (nl.at[theirs], NST.at[1]),
        (w1e, W1E.at[:, :, tp]), (el.at[theirs], E1.at[:, 0]), (w2e, W2E.at[:, tp]),
        (el.at[mine], E0.at[:, tp]), (w1n, W1N.at[:, :, tp]), (w2n, W2N.at[:, tp]),
        (ge.at[theirs], E1.at[:, 1]), (ge.at[mine], DE.at[:, tp]),
        (gn.at[mine], NST.at[2]), (gn.at[theirs], NST.at[3]),
    ]
    loads = [pltpu.make_async_copy(src, dst, lsem.at[i]) for i, (src, dst) in enumerate(loads)]
    for cp in loads:
        cp.start()

    barrier = pltpu.get_barrier_semaphore()
    pl.semaphore_signal(barrier, inc=1, device_id=partner, device_id_type=MESH)

    for base, ids in ((0, snd), (NP, rcv)):
        rows = lax.broadcasted_iota(jnp.int32, (NP, NE), 0)
        TT[base:base + NP] = jnp.where(rows == ids[...], 1.0, 0.0).astype(BF)
    row_i = lax.broadcasted_iota(jnp.int32, (NP, 3 * NP), 0)
    col_i = lax.broadcasted_iota(jnp.int32, (NP, 3 * NP), 1)
    eye3 = jnp.where((col_i == row_i) | (col_i == row_i + NP) | (col_i == row_i + 2 * NP), 1.0, 0.0).astype(BF)
    S3[...] = dot(TT[0:NP], eye3, 0, 0).astype(BF)
    R3[...] = dot(TT[NP:2 * NP], eye3, 0, 0).astype(BF)
    VF[...] = jnp.zeros_like(VF)
    DN[...] = jnp.zeros_like(DN)

    pl.semaphore_wait(barrier, 1)
    vec_copies = [rdma(vece, VE.at[tp], 0), rdma(vecn, VN.at[tp], 1)]
    for cp in vec_copies:
        cp.start()
    VE[tp] = vece[...]
    VN[tp] = vecn[...]

    loads[0].wait()
    loads[1].wait()
    NF[0] = NST[1].astype(F32)
    node_x = rdma(NF.at[0], NF.at[1], 2)
    node_x.start()

    def wblock(buf, layer, j):
        return buf.at[(layer * 7 + j) // 7, 0 if True else 0]

    def w_pack(layer, j):
        if j == J_NW2:
            half = W2N[layer, tp]
        elif j == J_EW2:
            half = W2E[layer, tp]
        elif j < J_EW2:
            return W1N[layer, j - J_NW1, tp].astype(F32)
        else:
            return W1E[layer, j - J_EW1, tp].astype(F32)
        half = half.astype(F32)
        return cat(half[0:H], half[H:2 * H])

    def w_unpack(layer, j, block):
        block = block.astype(BF)
        if j in (J_NW2, J_EW2):
            ref = W2N if j == J_NW2 else W2E
            ref[layer, ot, 0:H] = block[:, 0:H]
            ref[layer, ot, H:2 * H] = block[:, H:2 * H]
        elif j < J_EW2:
            W1N[layer, j - J_NW1, ot] = block
        else:
            W1E[layer, j - J_EW1, ot] = block

    def w_copy(layer, j):
        return rdma(G.at[1, layer, j], G.at[0, layer, j], 8 + layer * 7 + j)

    def w_send(layer, j):
        G[1, layer, j] = w_pack(layer, j)
        w_copy(layer, j).start()

    def w_recv(layer, j):
        w_copy(layer, j).wait()
        w_unpack(layer, j, G[0, layer, j])

    def lat_copy(b):
        return rdma(HS.at[b, :, 0:H], CS.at[b, :, 0:H], 32 + b)

    def grad_copy(b):
        return rdma(R2.at[b, :, 0:H], R2.at[b, :, H:D], 40 + b)

    loads[2].wait()
    for j in (5, 6, 4):
        w_send(0, j)
    loads[3].wait()
    loads[4].wait()

    def lat_send(b, carry):
        HS[b, :, 0:H] = E1[b, 0].astype(F32)
        lat_copy(b).start()
        return carry

    lax.fori_loop(0, 2, lat_send, 0)
    w_send(0, J_EW2)
    lax.fori_loop(2, NS, lat_send, 0)
    loads[6].wait()
    loads[7].wait()
    for j in (1, 2, 0):
        w_send(0, j)
    for j in (5, 6, 4, 3, 1, 2, 0):
        w_send(1, j)

    loads[8].wait()

    def grad_send(b, carry):
        R2[b, :, 0:H] = E1[b, 1].astype(F32)
        grad_copy(b).start()
        return carry

    lax.fori_loop(0, NS, grad_send, 0)
    loads[10].wait()
    loads[11].wait()
    NF[2] = NST[3].astype(F32)
    node_g = rdma(NF.at[2], NF.at[3], 3)
    node_g.start()

    def node_in(dst, staged, received):
        for b in range(NS):
            own, got = NST[staged, b], NF[received, b].astype(BF)
            lo = jnp.where(tp == 0, own, got)
            hi = jnp.where(tp == 0, got, own)
            dst[b * NP:b * NP + NN] = cat(lo, hi)

    for cp in vec_copies:
        cp.wait()
    node_x.wait()
    node_in(VF.at[0], 0, 1)

    def vec_row(layer, row, node):
        ref = VN if node else VE
        return cat(ref[0, layer, row:row + 1], ref[1, layer, row:row + 1])

    def put3(dst, value):
        parts = split3(value)
        for b in range(NS):
            for k in range(3):
                dst[b, k * NP:(k + 1) * NP] = parts[k][b * NP:(b + 1) * NP]

    def full1(ref, layer, k):
        return ref[layer, k].reshape(D, D)

    def gate(hidden):
        return 0.5 + 0.5 * jnp.tanh(0.5 * hidden)

    def second(act, ref, layer):
        return cat(dot(act, ref[layer, 0]), dot(act, ref[layer, 1]))

    def second_t(dout, ref, layer):
        return dot(dout[:, 0:H], ref[layer, 0], 1, 1) + dot(dout[:, H:D], ref[layer, 1], 1, 1)

    def layer_fwd(layer, src, dst):
        if layer == 0:
            w_recv(0, 5)
            w_recv(0, 6)
        put3(PS, dot(VF[layer], full1(W1E, layer, 1)))
        put3(PR, dot(VF[layer], full1(W1E, layer, 2)))
        if layer == 0:
            w_recv(0, 4)
            w_recv(0, 3)
            loads[5].wait()
        bias = b1e[layer:layer + 1]
        c0, gam, bet = (vec_row(layer, r, False) for r in range(3))

        def edge(b, carry):
            if layer == 0:
                lat_copy(b).wait()
                src[b, ot] = CS[b, :, 0:H].astype(BF)
            lat = cat(src[b, 0], src[b, 1])
            hidden = dot(lat, full1(W1E, layer, 0)) + dot(S3[...], PS[b]) + dot(R3[...], PR[b]) + bias
            HS[b] = hidden
            act = (hidden * gate(hidden)).astype(BF)
            out = second(act, W2E, layer) + c0
            cen = out - mean_cols(out)
            CS[b] = cen
            normed, unused = norm_parts(cen)
            msg = (normed * gam + bet).astype(BF)
            SF[layer, pl.ds(pl.multiple_of(b * NP, NP), NP)] = dot(TT[NP:2 * NP], msg).astype(BF)
            new = (lat.astype(F32) + msg.astype(F32)).astype(BF)
            dst[b, 0] = new[:, 0:H]
            dst[b, 1] = new[:, H:D]
            return carry

        lax.fori_loop(0, NS, edge, 0)
        if layer == 0:
            for cp in spills:
                cp.start()
            for j in (1, 2, 0):
                w_recv(0, j)
        lat = VF[layer]
        hidden = dot(lat, full1(W1N, layer, 0)) + dot(SF[layer], full1(W1N, layer, 1)) + b1n[layer:layer + 1]
        HN[layer] = hidden
        act = (hidden * gate(hidden)).astype(BF)
        out = second(act, W2N, layer) + vec_row(layer, 0, True)
        cen = out - mean_cols(out)
        CN[layer] = cen
        normed, unused = norm_parts(cen)
        msg = (normed * vec_row(layer, 1, True) + vec_row(layer, 2, True)).astype(BF)
        VF[layer + 1] = (lat.astype(F32) + msg.astype(F32)).astype(BF)

    spills = [pltpu.make_async_copy(HS, spill.at[0], spsem.at[0]), pltpu.make_async_copy(CS, spill.at[1], spsem.at[1])]
    fills = [pltpu.make_async_copy(spill.at[0], HS, spsem.at[2]), pltpu.make_async_copy(spill.at[1], CS, spsem.at[3])]

    layer_fwd(0, E0, E1)
    for j in range(7):
        w_recv(1, j)
    loads[9].wait()
    for b in range(NS):
        grad_copy(b).wait()
        DE[b, ot] = R2[b, :, H:D].astype(BF)
    node_g.wait()
    node_in(DN, 2, 3)
    for cp in spills:
        cp.wait()
    layer_fwd(1, E1, E2)

    def put_w2(layer, j, half, value, add):
        if add:
            G[layer, half, j, :, 0:H] += value[0:H]
            G[layer, half, j, :, H:D] += value[H:D]
        else:
            G[layer, half, j, :, 0:H] = value[0:H]
            G[layer, half, j, :, H:D] = value[H:D]

    def put_w1(layer, j, value, add):
        for half in range(2):
            if add:
                G[layer, half, j] += value[half * H:(half + 1) * H]
            else:
                G[layer, half, j] = value[half * H:(half + 1) * H]

    def mlp_bwd(d_msg, cen, hidden, gam, w2, layer, sm, j2, add):
        normed, inv_std = norm_parts(cen)
        sums = [sum_rows(d_msg * normed), sum_rows(d_msg)]
        d_normed = d_msg * gam
        d_out = inv_std * (d_normed - mean_cols(d_normed) - normed * mean_cols(d_normed * normed))
        sums = [sum_rows(d_out)] + sums
        d_out_bf = d_out.astype(BF)
        sig = gate(hidden)
        act = (hidden * sig).astype(BF)
        for half in range(2):
            put_w2(layer, j2, half, dot(act, d_out_bf[:, half * H:(half + 1) * H], 0, 0), add)
        d_hidden = second_t(d_out_bf, w2, layer) * (sig * (1.0 + hidden * (1.0 - sig)))
        sums = [sum_rows(d_hidden)] + sums
        for k in range(4):
            if add:
                SM[sm + k:sm + k + 1] += sums[k]
            else:
                SM[sm + k:sm + k + 1] = sums[k]
        return d_hidden.astype(BF)

    SM[...] = jnp.zeros_like(SM)

    def layer_bwd(layer, src):
        d_node = DN[...].astype(F32)
        d_hid = mlp_bwd(d_node, CN[layer], HN[layer], vec_row(layer, 1, True), W2N, layer, layer * 8, J_NW2, False)
        put_w1(layer, J_NW1, dot(VF[layer], d_hid, 0, 0), False)
        put_w1(layer, J_NW1 + 1, dot(SF[layer], d_hid, 0, 0), False)
        DV[...] = d_node + dot(d_hid, full1(W1N, layer, 0), 1, 1)
        put3(PS, dot(d_hid, full1(W1N, layer, 1), 1, 1))
        for j in (J_EW2, J_EW1):
            G[layer, :, j] = jnp.zeros((2, H, D), F32)
        gam = vec_row(layer, 1, False)
        if layer == 0:
            for cp in fills:
                cp.wait()

        def edge(b, carry):
            d_edge = cat(DE[b, 0], DE[b, 1]).astype(F32)
            d_msg = d_edge + dot(R3[...], PS[b])
            d_hid = mlp_bwd(d_msg, CS[b], HS[b], gam, W2E, layer, layer * 8 + 4, J_EW2, True)
            lat = cat(src[b, 0], src[b, 1])
            put_w1(layer, J_EW1, dot(lat, d_hid, 0, 0), True)
            new = (d_edge + dot(d_hid, full1(W1E, layer, 0), 1, 1)).astype(BF)
            DE[b, 0] = new[:, 0:H]
            DE[b, 1] = new[:, H:D]
            both = dot(TT[...], d_hid).astype(BF)
            at = pl.ds(pl.multiple_of(b * NP, NP), NP)
            GS[at] = both[0:NP]
            GR[at] = both[NP:2 * NP]
            return carry

        lax.fori_loop(0, NS, edge, 0)
        if layer == 1:
            for cp in fills:
                cp.start()
        put_w1(layer, J_EW1 + 1, dot(VF[layer], GS[...], 0, 0), False)
        put_w1(layer, J_EW1 + 2, dot(VF[layer], GR[...], 0, 0), False)
        DN[...] = (DV[...] + dot(GS[...], full1(W1E, layer, 1), 1, 1)
                   + dot(GR[...], full1(W1E, layer, 2), 1, 1)).astype(BF)

    layer_bwd(1, E1)
    layer_bwd(0, E0)

    pl.semaphore_signal(csem, inc=1, device_id=partner, device_id_type=MESH)
    for b in range(NS):
        at = slice(b * NP, b * NP + NN)
        for k, ref in ((0, VF.at[2]), (1, DN)):
            rows = ref[at]
            NST[2 * k, b] = jnp.where(tp == 0, rows[:, 0:H], rows[:, H:D])
            NF[2 * k, b] = jnp.where(tp == 0, rows[:, H:D], rows[:, 0:H]).astype(F32)

    def out_stage(b, carry):
        HS[b, :, 0:H] = E2[b, ot].astype(F32)
        HS[b, :, H:D] = DE[b, ot].astype(F32)
        return carry

    lax.fori_loop(0, NS, out_stage, 0)
    pl.semaphore_wait(csem, 1)
    node_o = [rdma(NF.at[0], NF.at[1], 4), rdma(NF.at[2], NF.at[3], 5)]
    for cp in node_o:
        cp.start()

    def out_copy(b):
        return rdma(HS.at[b], CS.at[b], 48 + b)

    for b in range(NS):
        out_copy(b).start()
    stores = [
        (E2.at[:, tp], o_e.at[mine]), (DE.at[:, tp], o_de.at[mine]),
        (NST.at[0], o_n.at[mine]), (NST.at[2], o_dn.at[mine]),
        (G, o_g), (SM, o_sm),
    ]
    stores = [pltpu.make_async_copy(src, dst, lsem.at[i]) for i, (src, dst) in enumerate(stores)]
    for cp in stores:
        cp.start()
    for k, cp in enumerate(node_o):
        cp.wait()
        NST[2 * k + 1] = NF[2 * k + 1].astype(BF)

    def out_recv(b, carry):
        out_copy(b).wait()
        E1[b, 0] = CS[b, :, 0:H].astype(BF)
        E1[b, 1] = CS[b, :, H:D].astype(BF)
        return carry

    lax.fori_loop(0, NS, out_recv, 0)
    more = [
        (E1.at[:, 0], o_e.at[theirs]), (E1.at[:, 1], o_de.at[theirs]),
        (NST.at[1], o_n.at[theirs]), (NST.at[3], o_dn.at[theirs]),
    ]
    more = [pltpu.make_async_copy(src, dst, lsem.at[6 + i]) for i, (src, dst) in enumerate(more)]
    for cp in more:
        cp.start()
    for cp in stores + more:
        cp.wait()


def compute(*args):
    any_spec = pl.BlockSpec(memory_space=pl.ANY)
    vm = pl.BlockSpec(memory_space=pltpu.VMEM)
    v = pltpu.VMEM
    lat = (2 * NS, NN, H)
    edg = (2 * NS, NE, H)
    outs = [(lat, BF), (edg, BF), (lat, BF), (edg, BF), ((2, 2, 7, H, D), F32), ((16, D), F32), ((2, NS, NE, D), F32)]
    scratch = [
        v((2, 3, 2, H, D), BF), v((2, 2, D, H), BF), v((2, 2, 2, H, D), BF), v((2, 2, D, H), BF),
        v((2, 2, 3, H), F32), v((2, 2, 3, H), F32),
        v((NE, 3 * NP), BF), v((NE, 3 * NP), BF), v((2 * NP, NE), BF),
        v((NS, 2, NE, H), BF), v((NS, 2, NE, H), BF), v((NS, 2, NE, H), BF), v((NS, 2, NE, H), BF),
        v((NS, NE, D), F32), v((NS, NE, D), F32), v((NS, NE, D), F32),
        v((2, 2, 7, H, D), F32), v((NS, 3 * NP, D), BF), v((NS, 3 * NP, D), BF),
        v((4, NS, NN, H), BF), v((4, NS, NN, H), F32),
        v((3, ROWS, D), BF), v((2, ROWS, D), BF), v((2, ROWS, D), F32), v((2, ROWS, D), F32),
        v((ROWS, D), BF), v((ROWS, D), F32), v((ROWS, D), BF), v((ROWS, D), BF), v((16, D), F32),
        pltpu.SemaphoreType.DMA((12,)), pltpu.SemaphoreType.DMA((56,)), pltpu.SemaphoreType.DMA((56,)),
        pltpu.SemaphoreType.REGULAR, pltpu.SemaphoreType.DMA((4,)),
    ]
    return pl.pallas_call(
        body,
        out_shape=[jax.ShapeDtypeStruct(*o) for o in outs],
        in_specs=[any_spec] * 8 + [vm] * 6,
        out_specs=[any_spec] * 7,
        scratch_shapes=scratch,
        compiler_params=pltpu.CompilerParams(
            collective_id=0, has_side_effects=True, vmem_limit_bytes=67043328),
    )(*args)


def solution(mesh):
    lat_spec = P('dp', None, 'tp')
    first_spec = P(None, None, 'tp', None)
    col_spec = P(None, None, 'tp')
    param_specs = (first_spec, P(), col_spec, col_spec, first_spec, P(), col_spec, col_spec)
    in_specs = (lat_spec, lat_spec, P(), P(), lat_spec, lat_spec) + param_specs
    out_specs = (lat_spec, lat_spec, lat_spec, lat_spec) + param_specs

    def local_step(node_lat, edge_lat, senders, receivers, grad_node, grad_edge, edge_w1, edge_b1, edge_w2, edge_vec, node_w1, node_b1, node_w2, node_vec):
        o_n, o_e, o_dn, o_de, grads, small, unused = compute(
            node_lat, edge_lat, grad_node, grad_edge, edge_w1, edge_w2, node_w1, node_w2,
            edge_b1, node_b1, edge_vec, node_vec, senders.reshape(1, NE), receivers.reshape(1, NE))
        grads = lax.psum_scatter(grads, 'tp', scatter_dimension=1, tiled=False)
        grads, small = lax.psum(grads, 'dp'), lax.psum(small, ('dp', 'tp'))
        small = small.reshape(2, 8, D)
        col = lax.axis_index('tp') * H

        def w2(j):
            block = grads[:, j]
            return jnp.concatenate([block[:, :, 0:H], block[:, :, H:D]], axis=1)

        def vec(row):
            return lax.dynamic_slice_in_dim(small[:, row:row + 3], col, H, axis=2)

        return (o_n, o_e, o_dn, o_de,
                grads[:, J_EW1:J_EW1 + 3], small[:, 4], w2(J_EW2), vec(5),
                grads[:, J_NW1:J_NW1 + 2], small[:, 0], w2(J_NW2), vec(1))

    return jax.shard_map(local_step, mesh=mesh, in_specs=in_specs, out_specs=out_specs, check_vma=False)
```

```python
import functools

import jax
import jax.numpy as jnp
from jax import lax
from jax.experimental import pallas as pl
from jax.experimental.pallas import tpu as pltpu
from jax.sharding import PartitionSpec as P

BF = jnp.bfloat16
F32 = jnp.float32
MESH = pl.DeviceIdType.MESH
LN_EPS = 1e-5
NS = 8
NN = 42
NE = 300
D = 512
H = 256
ROWS = NN * NS
NB = 10
BE = NE // NB
BR = BE * NS


def dot(lhs, rhs, lc=1, rc=0):
    return lax.dot_general(lhs, rhs, (((lc,), (rc,)), ((), ())), preferred_element_type=F32)


def cat(lhs, rhs):
    return jnp.concatenate([lhs, rhs], axis=1)


def mean_cols(x):
    return jnp.sum(x, axis=1, keepdims=True) * (1.0 / D)


def sum_rows(x):
    return jnp.sum(x, axis=0, keepdims=True)


def norm_parts(centered):
    inv_std = lax.rsqrt(mean_cols(centered * centered) + LN_EPS)
    return centered * inv_std, inv_std


J_NW2, J_NW1, J_EW2, J_EW1 = 0, 1, 3, 4


def rows_of(block):
    return block.astype(F32).reshape(block.shape[0] * NS, block.shape[2])


def body(nl, el, gn, ge, w1e, w2e, w1n, w2n, b1e, b1n, vece, vecn, flat, snd, rcv,
         o_n, o_e, o_dn, o_de, o_g, o_sm, spill,
         W1E, W2E, W1N, W2N, VE, VN, KS, KR,
         E0, E1, E2, DE, HS, CS, R2, G, PS, PR, GA, AG,
         NST, NF, VF, SF, HN, CN, DN, DV, SM,
         lsem, ssem, rsem, csem, spsem):
    dp = lax.axis_index('dp')
    tp = lax.axis_index('tp')
    ot = 1 - tp
    partner = (dp, ot)

    def rdma(src, dst, idx):
        return pltpu.make_async_remote_copy(
            src_ref=src, dst_ref=dst, send_sem=ssem.at[idx], recv_sem=rsem.at[idx],
            device_id=partner, device_id_type=MESH)

    mine = pl.ds(pl.multiple_of(tp * NS, NS), NS)
    theirs = pl.ds(pl.multiple_of(ot * NS, NS), NS)
    loads = [
        (nl.at[:, mine], NST.at[0]), (nl.at[:, theirs], NST.at[1]),
        (w1e, W1E.at[:, :, tp]), (el.at[:, theirs], E1.at[0]), (w2e, W2E.at[:, tp]),
        (el.at[:, mine], E0.at[tp]), (w1n, W1N.at[:, :, tp]), (w2n, W2N.at[:, tp]),
        (ge.at[:, theirs], E1.at[1]), (ge.at[:, mine], DE.at[tp]),
        (gn.at[:, mine], NST.at[2]), (gn.at[:, theirs], NST.at[3]),
    ]
    loads = [pltpu.make_async_copy(src, dst, lsem.at[i]) for i, (src, dst) in enumerate(loads)]
    for cp in loads:
        cp.start()

    barrier = pltpu.get_barrier_semaphore()
    pl.semaphore_signal(barrier, inc=1, device_id=partner, device_id_type=MESH)

    pl.semaphore_wait(barrier, 1)
    vec_copies = [rdma(vece, VE.at[tp], 0), rdma(vecn, VN.at[tp], 1)]
    for cp in vec_copies:
        cp.start()
    VE[tp] = vece[...]
    VN[tp] = vecn[...]

    loads[0].wait()
    loads[1].wait()
    NF[0] = NST[1].astype(F32)
    node_x = rdma(NF.at[0], NF.at[1], 2)
    node_x.start()

    def w_pack(layer, j):
        if j == J_NW2:
            half = W2N[layer, tp]
        elif j == J_EW2:
            half = W2E[layer, tp]
        elif j < J_EW2:
            return W1N[layer, j - J_NW1, tp].astype(F32)
        else:
            return W1E[layer, j - J_EW1, tp].astype(F32)
        half = half.astype(F32)
        return cat(half[0:H], half[H:2 * H])

    def w_unpack(layer, j, block):
        block = block.astype(BF)
        if j in (J_NW2, J_EW2):
            ref = W2N if j == J_NW2 else W2E
            ref[layer, ot, 0:H] = block[:, 0:H]
            ref[layer, ot, H:2 * H] = block[:, H:2 * H]
        elif j < J_EW2:
            W1N[layer, j - J_NW1, ot] = block
        else:
            W1E[layer, j - J_EW1, ot] = block

    def w_copy(layer, j):
        return rdma(G.at[1, layer, j], G.at[0, layer, j], 8 + layer * 7 + j)

    def w_send(layer, j):
        G[1, layer, j] = w_pack(layer, j)
        w_copy(layer, j).start()

    def w_recv(layer, j):
        w_copy(layer, j).wait()
        w_unpack(layer, j, G[0, layer, j])

    def edges(b):
        return pl.ds(b * BE, BE)

    def erows(b):
        return pl.ds(pl.multiple_of(b * BR, BR), BR)

    def lat_copy(b):
        return rdma(HS.at[erows(b), 0:H], CS.at[erows(b), 0:H], 24 + b)

    def grad_copy(b):
        return rdma(R2.at[erows(b), 0:H], R2.at[erows(b), H:D], 34 + b)

    loads[2].wait()
    for j in (5, 6, 4):
        w_send(0, j)
    loads[3].wait()
    loads[4].wait()

    def lat_send(b, carry):
        HS[erows(b), 0:H] = rows_of(E1[0, edges(b)])
        lat_copy(b).start()
        return carry

    lat_send(0, 0)
    w_send(0, J_EW2)
    lax.fori_loop(1, NB, lat_send, 0)
    loads[6].wait()
    loads[7].wait()
    for j in (1, 2, 0):
        w_send(0, j)
    for j in (5, 6, 4, 3, 1, 2, 0):
        w_send(1, j)

    loads[8].wait()

    def grad_send(b, carry):
        R2[erows(b), 0:H] = rows_of(E1[1, edges(b)])
        grad_copy(b).start()
        return carry

    lax.fori_loop(0, NB, grad_send, 0)
    loads[10].wait()
    loads[11].wait()
    NF[2] = NST[3].astype(F32)
    node_g = rdma(NF.at[2], NF.at[3], 3)
    node_g.start()

    def select(dst, base):
        def one(b, carry):
            rows = lax.broadcasted_iota(jnp.int32, (ROWS, BR), 0)
            dst[b] = jnp.where(rows == flat[base + b], 1.0, 0.0).astype(BF)
            return carry
        lax.fori_loop(0, NB, one, 0)

    select(KR, NB)
    select(KS, 0)

    def node_in(dst, staged, received):
        own, got = rows_of(NST[staged]), rows_of(NF[received])
        lo = jnp.where(tp == 0, own, got)
        hi = jnp.where(tp == 0, got, own)
        dst[...] = cat(lo, hi).astype(BF)

    for cp in vec_copies:
        cp.wait()
    node_x.wait()
    node_in(VF.at[0], 0, 1)

    def vec_row(layer, row, node):
        ref = VN if node else VE
        return cat(ref[0, row, layer:layer + 1], ref[1, row, layer:layer + 1])

    def full1(ref, layer, k):
        return ref[layer, k].reshape(D, D)

    def gate(hidden):
        return 0.5 + 0.5 * jnp.tanh(0.5 * hidden)

    def second(act, ref, layer):
        return cat(dot(act, ref[layer, 0]), dot(act, ref[layer, 1]))

    def second_t(dout, ref, layer):
        return dot(dout[:, 0:H], ref[layer, 0], 1, 1) + dot(dout[:, H:D], ref[layer, 1], 1, 1)

    def layer_fwd(layer, src, dst):
        if layer == 0:
            w_recv(0, 5)
            w_recv(0, 6)
        PS[...] = (dot(VF[layer], full1(W1E, layer, 1)) + b1e[layer:layer + 1]).reshape(NN, NS, D)
        PR[...] = dot(VF[layer], full1(W1E, layer, 2)).reshape(NN, NS, D)
        if layer == 0:
            w_recv(0, 4)
            w_recv(0, 3)
            loads[5].wait()
        c0, gam, bet = (vec_row(layer, r, False) for r in range(3))
        AG[...] = jnp.zeros_like(AG)

        def edge(b, carry):
            if layer == 0:
                lat_copy(b).wait()
                src[ot, edges(b)] = CS[erows(b), 0:H].reshape(BE, NS, H).astype(BF)
            for i in range(BE):
                GA[i * NS:(i + 1) * NS] = PS[snd[b * BE + i]] + PR[rcv[b * BE + i]]
            lat = cat(rows_of(src[0, edges(b)]), rows_of(src[1, edges(b)]))
            hidden = dot(lat.astype(BF), full1(W1E, layer, 0)) + GA[...]
            HS[erows(b)] = hidden
            act = (hidden * gate(hidden)).astype(BF)
            out = second(act, W2E, layer) + c0
            cen = out - mean_cols(out)
            CS[erows(b)] = cen
            normed, unused = norm_parts(cen)
            msg = (normed * gam + bet).astype(BF)
            AG[...] += dot(KR[b], msg)
            new = lat + msg.astype(F32)
            dst[0, edges(b)] = new[:, 0:H].reshape(BE, NS, H).astype(BF)
            dst[1, edges(b)] = new[:, H:D].reshape(BE, NS, H).astype(BF)
            return carry

        lax.fori_loop(0, NB, edge, 0)
        if layer == 0:
            for cp in spills:
                cp.start()
            for j in (1, 2, 0):
                w_recv(0, j)
        SF[layer] = AG[...].astype(BF)
        lat = VF[layer]
        hidden = dot(lat, full1(W1N, layer, 0)) + dot(SF[layer], full1(W1N, layer, 1)) + b1n[layer:layer + 1]
        HN[layer] = hidden
        act = (hidden * gate(hidden)).astype(BF)
        out = second(act, W2N, layer) + vec_row(layer, 0, True)
        cen = out - mean_cols(out)
        CN[layer] = cen
        normed, unused = norm_parts(cen)
        msg = (normed * vec_row(layer, 1, True) + vec_row(layer, 2, True)).astype(BF)
        VF[layer + 1] = (lat.astype(F32) + msg.astype(F32)).astype(BF)

    spills = [pltpu.make_async_copy(HS, spill.at[0], spsem.at[0]), pltpu.make_async_copy(CS, spill.at[1], spsem.at[1])]
    fills = [pltpu.make_async_copy(spill.at[0], HS, spsem.at[2]), pltpu.make_async_copy(spill.at[1], CS, spsem.at[3])]

    layer_fwd(0, E0, E1)
    for j in range(7):
        w_recv(1, j)
    loads[9].wait()

    def grad_recv(b, carry):
        grad_copy(b).wait()
        DE[ot, edges(b)] = R2[erows(b), H:D].reshape(BE, NS, H).astype(BF)
        return carry

    lax.fori_loop(0, NB, grad_recv, 0)
    node_g.wait()
    node_in(DN, 2, 3)
    for cp in spills:
        cp.wait()
    layer_fwd(1, E1, E2)

    def put_w2(layer, j, half, value, add):
        if add:
            G[layer, half, j, :, 0:H] += value[0:H]
            G[layer, half, j, :, H:D] += value[H:D]
        else:
            G[layer, half, j, :, 0:H] = value[0:H]
            G[layer, half, j, :, H:D] = value[H:D]

    def put_w1(layer, j, value, add):
        for half in range(2):
            if add:
                G[layer, half, j] += value[half * H:(half + 1) * H]
            else:
                G[layer, half, j] = value[half * H:(half + 1) * H]

    def mlp_bwd(d_msg, cen, hidden, gam, w2, layer, sm, j2, add):
        normed, inv_std = norm_parts(cen)
        sums = [sum_rows(d_msg * normed), sum_rows(d_msg)]
        d_normed = d_msg * gam
        d_out = inv_std * (d_normed - mean_cols(d_normed) - normed * mean_cols(d_normed * normed))
        sums = [sum_rows(d_out)] + sums
        d_out_bf = d_out.astype(BF)
        sig = gate(hidden)
        act = (hidden * sig).astype(BF)
        for half in range(2):
            put_w2(layer, j2, half, dot(act, d_out_bf[:, half * H:(half + 1) * H], 0, 0), add)
        d_hidden = second_t(d_out_bf, w2, layer) * (sig * (1.0 + hidden * (1.0 - sig)))
        sums = [sum_rows(d_hidden)] + sums
        for k in range(4):
            if add:
                SM[sm + k:sm + k + 1] += sums[k]
            else:
                SM[sm + k:sm + k + 1] = sums[k]
        return d_hidden.astype(BF)

    SM[...] = jnp.zeros_like(SM)

    def layer_bwd(layer, src):
        d_node = DN[...].astype(F32)
        d_hid = mlp_bwd(d_node, CN[layer], HN[layer], vec_row(layer, 1, True), W2N, layer, layer * 8, J_NW2, False)
        put_w1(layer, J_NW1, dot(VF[layer], d_hid, 0, 0), False)
        put_w1(layer, J_NW1 + 1, dot(SF[layer], d_hid, 0, 0), False)
        DV[...] = d_node + dot(d_hid, full1(W1N, layer, 0), 1, 1)
        PS[...] = dot(d_hid, full1(W1N, layer, 1), 1, 1).reshape(NN, NS, D)
        for j in (J_EW2, J_EW1):
            G[layer, :, j] = jnp.zeros((2, H, D), F32)
        AG[...] = jnp.zeros_like(AG)
        PR[...] = jnp.zeros_like(PR)
        gam = vec_row(layer, 1, False)
        if layer == 0:
            for cp in fills:
                cp.wait()

        def edge(b, carry):
            for i in range(BE):
                GA[i * NS:(i + 1) * NS] = PS[rcv[b * BE + i]]
            d_edge = cat(rows_of(DE[0, edges(b)]), rows_of(DE[1, edges(b)]))
            d_hid = mlp_bwd(d_edge + GA[...], CS[erows(b)], HS[erows(b)], gam, W2E, layer, layer * 8 + 4, J_EW2, True)
            lat = cat(rows_of(src[0, edges(b)]), rows_of(src[1, edges(b)])).astype(BF)
            put_w1(layer, J_EW1, dot(lat, d_hid, 0, 0), True)
            new = d_edge + dot(d_hid, full1(W1E, layer, 0), 1, 1)
            DE[0, edges(b)] = new[:, 0:H].reshape(BE, NS, H).astype(BF)
            DE[1, edges(b)] = new[:, H:D].reshape(BE, NS, H).astype(BF)
            AG[...] += dot(KS[b], d_hid)
            PR[...] += dot(KR[b], d_hid).reshape(NN, NS, D)
            return carry

        lax.fori_loop(0, NB, edge, 0)
        if layer == 1:
            for cp in fills:
                cp.start()
        d_ps, d_pr = AG[...].astype(BF), rows_of(PR[...]).astype(BF)
        put_w1(layer, J_EW1 + 1, dot(VF[layer], d_ps, 0, 0), False)
        put_w1(layer, J_EW1 + 2, dot(VF[layer], d_pr, 0, 0), False)
        DN[...] = (DV[...] + dot(d_ps, full1(W1E, layer, 1), 1, 1)
                   + dot(d_pr, full1(W1E, layer, 2), 1, 1)).astype(BF)

    layer_bwd(1, E1)
    layer_bwd(0, E0)

    pl.semaphore_signal(csem, inc=1, device_id=partner, device_id_type=MESH)
    for k, ref in ((0, VF.at[2]), (1, DN)):
        rows = ref[...].astype(F32)
        NST[2 * k] = jnp.where(tp == 0, rows[:, 0:H], rows[:, H:D]).reshape(NN, NS, H).astype(BF)
        NF[2 * k] = jnp.where(tp == 0, rows[:, H:D], rows[:, 0:H]).reshape(NN, NS, H)

    def out_stage(b, carry):
        HS[erows(b), 0:H] = rows_of(E2[ot, edges(b)])
        HS[erows(b), H:D] = rows_of(DE[ot, edges(b)])
        return carry

    lax.fori_loop(0, NB, out_stage, 0)
    pl.semaphore_wait(csem, 1)
    node_o = [rdma(NF.at[0], NF.at[1], 4), rdma(NF.at[2], NF.at[3], 5)]
    for cp in node_o:
        cp.start()

    def out_copy(b):
        return rdma(HS.at[erows(b)], CS.at[erows(b)], 44 + b)

    for b in range(NB):
        out_copy(b).start()
    stores = [
        (E2.at[tp], o_e.at[:, mine]), (DE.at[tp], o_de.at[:, mine]),
        (NST.at[0], o_n.at[:, mine]), (NST.at[2], o_dn.at[:, mine]),
        (G, o_g), (SM, o_sm),
    ]
    stores = [pltpu.make_async_copy(src, dst, lsem.at[i]) for i, (src, dst) in enumerate(stores)]
    for cp in stores:
        cp.start()
    for k, cp in enumerate(node_o):
        cp.wait()
        NST[2 * k + 1] = NF[2 * k + 1].astype(BF)

    def out_recv(b, carry):
        out_copy(b).wait()
        E1[0, edges(b)] = CS[erows(b), 0:H].reshape(BE, NS, H).astype(BF)
        E1[1, edges(b)] = CS[erows(b), H:D].reshape(BE, NS, H).astype(BF)
        return carry

    lax.fori_loop(0, NB, out_recv, 0)
    more = [
        (E1.at[0], o_e.at[:, theirs]), (E1.at[1], o_de.at[:, theirs]),
        (NST.at[1], o_n.at[:, theirs]), (NST.at[3], o_dn.at[:, theirs]),
    ]
    more = [pltpu.make_async_copy(src, dst, lsem.at[6 + i]) for i, (src, dst) in enumerate(more)]
    for cp in more:
        cp.start()
    for cp in stores + more:
        cp.wait()


def compute(*args):
    any_spec = pl.BlockSpec(memory_space=pl.ANY)
    vm = pl.BlockSpec(memory_space=pltpu.VMEM)
    sm = pl.BlockSpec(memory_space=pltpu.SMEM)
    v = pltpu.VMEM
    lat = (NN, 2 * NS, H)
    edg = (NE, 2 * NS, H)
    outs = [(lat, BF), (edg, BF), (lat, BF), (edg, BF), ((2, 2, 7, H, D), F32), ((16, D), F32), ((2, NE * NS, D), F32)]
    scratch = [
        v((2, 3, 2, H, D), BF), v((2, 2, D, H), BF), v((2, 2, 2, H, D), BF), v((2, 2, D, H), BF),
        v((2, 3, 2, H), F32), v((2, 3, 2, H), F32),
        v((NB, ROWS, BR), BF), v((NB, ROWS, BR), BF),
        v((2, NE, NS, H), BF), v((2, NE, NS, H), BF), v((2, NE, NS, H), BF), v((2, NE, NS, H), BF),
        v((NE * NS, D), F32), v((NE * NS, D), F32), v((NE * NS, D), F32),
        v((2, 2, 7, H, D), F32), v((NN, NS, D), F32), v((NN, NS, D), F32), v((BR, D), F32), v((ROWS, D), F32),
        v((4, NN, NS, H), BF), v((4, NN, NS, H), F32),
        v((3, ROWS, D), BF), v((2, ROWS, D), BF), v((2, ROWS, D), F32), v((2, ROWS, D), F32),
        v((ROWS, D), BF), v((ROWS, D), F32), v((16, D), F32),
        pltpu.SemaphoreType.DMA((12,)), pltpu.SemaphoreType.DMA((56,)), pltpu.SemaphoreType.DMA((56,)),
        pltpu.SemaphoreType.REGULAR, pltpu.SemaphoreType.DMA((4,)),
    ]
    return pl.pallas_call(
        body,
        out_shape=[jax.ShapeDtypeStruct(*o) for o in outs],
        in_specs=[any_spec] * 8 + [vm] * 5 + [sm] * 2,
        out_specs=[any_spec] * 7,
        scratch_shapes=scratch,
        compiler_params=pltpu.CompilerParams(
            collective_id=0, has_side_effects=True, vmem_limit_bytes=67043328),
    )(*args)


def solution(mesh):
    lat_spec = P('dp', None, 'tp')
    first_spec = P(None, None, 'tp', None)
    col_spec = P(None, None, 'tp')
    param_specs = (first_spec, P(), col_spec, col_spec, first_spec, P(), col_spec, col_spec)
    in_specs = (lat_spec, lat_spec, P(), P(), lat_spec, lat_spec) + param_specs
    out_specs = (lat_spec, lat_spec, lat_spec, lat_spec) + param_specs

    def local_step(node_lat, edge_lat, senders, receivers, grad_node, grad_edge, edge_w1, edge_b1, edge_w2, edge_vec, node_w1, node_b1, node_w2, node_vec):
        def swap(x):
            return jnp.transpose(x, (1, 0, 2))

        ids = jnp.stack([senders, receivers])
        flat = ids[:, :, None] * NS + jnp.arange(NS, dtype=jnp.int32)
        o_n, o_e, o_dn, o_de, grads, small, unused = compute(
            swap(node_lat), swap(edge_lat), swap(grad_node), swap(grad_edge), edge_w1, edge_w2, node_w1, node_w2,
            edge_b1, node_b1, swap(edge_vec), swap(node_vec), flat.reshape(2 * NB, 1, BR), senders, receivers)
        o_n, o_e, o_dn, o_de = swap(o_n), swap(o_e), swap(o_dn), swap(o_de)
        grads = lax.psum_scatter(grads, 'tp', scatter_dimension=1, tiled=False)
        grads, small = lax.psum(grads, 'dp'), lax.psum(small, ('dp', 'tp'))
        small = small.reshape(2, 8, D)
        col = lax.axis_index('tp') * H

        def w2(j):
            block = grads[:, j]
            return jnp.concatenate([block[:, :, 0:H], block[:, :, H:D]], axis=1)

        def vec(row):
            return lax.dynamic_slice_in_dim(small[:, row:row + 3], col, H, axis=2)

        return (o_n, o_e, o_dn, o_de,
                grads[:, J_EW1:J_EW1 + 3], small[:, 4], w2(J_EW2), vec(5),
                grads[:, J_NW1:J_NW1 + 2], small[:, 0], w2(J_NW2), vec(1))

    return jax.shard_map(local_step, mesh=mesh, in_specs=in_specs, out_specs=out_specs, check_vma=False)
```

```python
import functools

import jax
import jax.numpy as jnp
from jax import lax
from jax.experimental import pallas as pl
from jax.experimental.pallas import tpu as pltpu
from jax.sharding import PartitionSpec as P

BF = jnp.bfloat16
F32 = jnp.float32
MESH = pl.DeviceIdType.MESH
LN_EPS = 1e-5
NS = 8
NN = 42
NE = 300
D = 512
H = 256
ROWS = NN * NS
NB = 10
BE = NE // NB
BR = BE * NS


def dot(lhs, rhs, lc=1, rc=0):
    return lax.dot_general(lhs, rhs, (((lc,), (rc,)), ((), ())), preferred_element_type=F32)


def dot_rows(lhs, rhs):
    return dot(lhs, rhs, 0, 0)


def dot_cols(lhs, rhs):
    return dot(lhs, rhs, 1, 1)


def cat(lhs, rhs):
    return jnp.concatenate([lhs, rhs], axis=1)


def mean_cols(x):
    return jnp.sum(x, axis=1, keepdims=True) * (1.0 / D)


def sum_rows(x):
    return jnp.sum(x, axis=0, keepdims=True)


def norm_parts(centered):
    inv_std = lax.rsqrt(mean_cols(centered * centered) + LN_EPS)
    return centered * inv_std, inv_std


J_NW2, J_NW1, J_EW2, J_EW1 = 0, 1, 3, 4


def rows_of(block):
    return block.astype(F32).reshape(block.shape[0] * NS, block.shape[2])


def body(nl, el, gn, ge, w1e, w2e, w1n, w2n, b1e, b1n, vece, vecn, flat, snd, rcv,
         o_n, o_e, o_dn, o_de, o_ew1, o_ew2, o_nw1, o_nw2, o_be, o_bn, o_ve, o_vn, spill,
         W1E, W2E, W1N, W2N, VE, VN, KS, KR,
         E0, E1, E2, DE, HS, CS, R2, G, PS, PR, GA, AG,
         NST, NF, VF, SF, HN, CN, DN, DV, SM,
         lsem, ssem, rsem, csem, spsem, gssem, grsem, osem):
    dp = lax.axis_index('dp')
    tp = lax.axis_index('tp')
    ot = 1 - tp
    partner = (dp, ot)
    cx, cy = lax.rem(dp, 2), dp // 2
    x_peer = (cy * 2 + 1 - cx, tp)
    y_peer = ((1 - cy) * 2 + cx, tp)
    peers = (partner, x_peer, y_peer)

    def rdma(src, dst, idx):
        return pltpu.make_async_remote_copy(
            src_ref=src, dst_ref=dst, send_sem=ssem.at[idx], recv_sem=rsem.at[idx],
            device_id=partner, device_id_type=MESH)

    mine = pl.ds(pl.multiple_of(tp * NS, NS), NS)
    theirs = pl.ds(pl.multiple_of(ot * NS, NS), NS)
    loads = [
        (nl.at[:, mine], NST.at[0]), (nl.at[:, theirs], NST.at[1]),
        (w1e, W1E.at[:, :, tp]), (el.at[:, theirs], E1.at[0]), (w2e, W2E.at[:, tp]),
        (el.at[:, mine], E0.at[tp]), (w1n, W1N.at[:, :, tp]), (w2n, W2N.at[:, tp]),
        (ge.at[:, theirs], E1.at[1]), (ge.at[:, mine], DE.at[tp]),
        (gn.at[:, mine], NST.at[2]), (gn.at[:, theirs], NST.at[3]),
    ]
    loads = [pltpu.make_async_copy(src, dst, lsem.at[i]) for i, (src, dst) in enumerate(loads)]
    for cp in loads:
        cp.start()

    barrier = pltpu.get_barrier_semaphore()
    for peer in peers:
        pl.semaphore_signal(barrier, inc=1, device_id=peer, device_id_type=MESH)
    pl.semaphore_wait(barrier, 3)
    vec_copies = [rdma(vece, VE.at[tp], 0), rdma(vecn, VN.at[tp], 1)]
    for cp in vec_copies:
        cp.start()
    VE[tp] = vece[...]
    VN[tp] = vecn[...]

    loads[0].wait()
    loads[1].wait()
    NF[0] = NST[1].astype(F32)
    node_x = rdma(NF.at[0], NF.at[1], 2)
    node_x.start()

    def w_pack(layer, j):
        if j == J_NW2:
            half = W2N[layer, tp]
        elif j == J_EW2:
            half = W2E[layer, tp]
        elif j < J_EW2:
            return W1N[layer, j - J_NW1, tp].astype(F32)
        else:
            return W1E[layer, j - J_EW1, tp].astype(F32)
        half = half.astype(F32)
        return cat(half[:H], half[H:])

    def w_unpack(layer, j, block):
        block = block.astype(BF)
        if j in (J_NW2, J_EW2):
            ref = W2N if j == J_NW2 else W2E
            ref[layer, ot, :H] = block[:, :H]
            ref[layer, ot, H:] = block[:, H:]
        elif j < J_EW2:
            W1N[layer, j - J_NW1, ot] = block
        else:
            W1E[layer, j - J_EW1, ot] = block

    def w_copy(layer, j):
        return rdma(G.at[1, layer, j], G.at[0, layer, j], 8 + layer * 7 + j)

    def w_send(layer, j):
        G[1, layer, j] = w_pack(layer, j)
        w_copy(layer, j).start()

    def w_recv(layer, j):
        w_copy(layer, j).wait()
        w_unpack(layer, j, G[0, layer, j])

    def edges(b):
        return pl.ds(b * BE, BE)

    def erows(b):
        return pl.ds(pl.multiple_of(b * BR, BR), BR)

    def lat_copy(b):
        return rdma(HS.at[erows(b), :H], CS.at[erows(b), :H], 24 + b)

    def grad_copy(b):
        return rdma(R2.at[erows(b), :H], R2.at[erows(b), H:], 34 + b)

    loads[2].wait()
    for j in (5, 6, 4):
        w_send(0, j)
    loads[3].wait()
    loads[4].wait()

    def lat_send(b, carry):
        HS[erows(b), :H] = rows_of(E1[0, edges(b)])
        lat_copy(b).start()
        return carry

    lat_send(0, 0)
    w_send(0, J_EW2)
    lax.fori_loop(1, NB, lat_send, 0)
    loads[6].wait()
    loads[7].wait()
    for j in (1, 2, 0):
        w_send(0, j)
    for j in (5, 6, 4, 3, 1, 2, 0):
        w_send(1, j)

    loads[8].wait()

    def grad_send(b, carry):
        R2[erows(b), :H] = rows_of(E1[1, edges(b)])
        grad_copy(b).start()
        return carry

    lax.fori_loop(0, NB, grad_send, 0)
    loads[10].wait()
    loads[11].wait()
    NF[2] = NST[3].astype(F32)
    node_g = rdma(NF.at[2], NF.at[3], 3)
    node_g.start()

    def select(dst, base):
        def one(b, carry):
            rows = lax.broadcasted_iota(jnp.int32, (ROWS, BR), 0)
            dst[b] = jnp.where(rows == flat[base + b], 1.0, 0.0).astype(BF)
            return carry
        lax.fori_loop(0, NB, one, 0)

    select(KR, NB)
    select(KS, 0)

    def node_in(dst, staged, received):
        own, got = rows_of(NST[staged]), rows_of(NF[received])
        lo = jnp.where(tp == 0, own, got)
        hi = jnp.where(tp == 0, got, own)
        dst[...] = cat(lo, hi).astype(BF)

    for cp in vec_copies:
        cp.wait()
    node_x.wait()
    node_in(VF.at[0], 0, 1)

    def vec_row(layer, row, node):
        ref = VN if node else VE
        return cat(ref[0, row, layer:layer + 1], ref[1, row, layer:layer + 1])

    def full1(ref, layer, k):
        return ref[layer, k].reshape(D, D)

    def gate(hidden):
        return 0.5 + 0.5 * jnp.tanh(0.5 * hidden)

    def second(act, ref, layer):
        return cat(dot(act, ref[layer, 0]), dot(act, ref[layer, 1]))

    def second_t(dout, ref, layer):
        return dot_cols(dout[:, :H], ref[layer, 0]) + dot_cols(dout[:, H:], ref[layer, 1])

    def layer_fwd(layer, src, dst):
        if layer == 0:
            w_recv(0, 5)
            w_recv(0, 6)
        PS[...] = (dot(VF[layer], full1(W1E, layer, 1)) + b1e[layer:layer + 1]).reshape(NN, NS, D)
        PR[...] = dot(VF[layer], full1(W1E, layer, 2)).reshape(NN, NS, D)
        if layer == 0:
            w_recv(0, 4)
            w_recv(0, 3)
            loads[5].wait()
        c0, gam, bet = (vec_row(layer, r, False) for r in range(3))
        AG[...] = jnp.zeros_like(AG)

        def edge(b, carry):
            if layer == 0:
                lat_copy(b).wait()
                src[ot, edges(b)] = CS[erows(b), :H].reshape(BE, NS, H).astype(BF)
            for i in range(BE):
                GA[i * NS:(i + 1) * NS] = PS[snd[b * BE + i]] + PR[rcv[b * BE + i]]
            lat = cat(rows_of(src[0, edges(b)]), rows_of(src[1, edges(b)]))
            hidden = dot(lat.astype(BF), full1(W1E, layer, 0)) + GA[...]
            HS[erows(b)] = hidden
            act = (hidden * gate(hidden)).astype(BF)
            out = second(act, W2E, layer) + c0
            cen = out - mean_cols(out)
            CS[erows(b)] = cen
            normed, unused = norm_parts(cen)
            msg = (normed * gam + bet).astype(BF)
            AG[...] += dot(KR[b], msg)
            new = lat + msg.astype(F32)
            dst[0, edges(b)] = new[:, :H].reshape(BE, NS, H).astype(BF)
            dst[1, edges(b)] = new[:, H:].reshape(BE, NS, H).astype(BF)
            return carry

        lax.fori_loop(0, NB, edge, 0)
        if layer == 0:
            for cp in spills:
                cp.start()
            for j in (1, 2, 0):
                w_recv(0, j)
        SF[layer] = AG[...].astype(BF)
        lat = VF[layer]
        hidden = dot(lat, full1(W1N, layer, 0)) + dot(SF[layer], full1(W1N, layer, 1)) + b1n[layer:layer + 1]
        HN[layer] = hidden
        act = (hidden * gate(hidden)).astype(BF)
        out = second(act, W2N, layer) + vec_row(layer, 0, True)
        cen = out - mean_cols(out)
        CN[layer] = cen
        normed, unused = norm_parts(cen)
        msg = (normed * vec_row(layer, 1, True) + vec_row(layer, 2, True)).astype(BF)
        VF[layer + 1] = (lat.astype(F32) + msg.astype(F32)).astype(BF)

    spills = [pltpu.make_async_copy(HS, spill.at[0], spsem.at[0]), pltpu.make_async_copy(CS, spill.at[1], spsem.at[1])]
    fills = [pltpu.make_async_copy(spill.at[0], HS, spsem.at[2]), pltpu.make_async_copy(spill.at[1], CS, spsem.at[3])]

    layer_fwd(0, E0, E1)
    for j in range(7):
        w_recv(1, j)
    loads[9].wait()

    def grad_recv(b, carry):
        grad_copy(b).wait()
        DE[ot, edges(b)] = R2[erows(b), H:].reshape(BE, NS, H).astype(BF)
        return carry

    lax.fori_loop(0, NB, grad_recv, 0)
    for peer in peers:
        pl.semaphore_signal(csem.at[0], inc=1, device_id=peer, device_id_type=MESH)
    node_g.wait()
    node_in(DN, 2, 3)
    for cp in spills:
        cp.wait()
    layer_fwd(1, E1, E2)

    def chunk(c):
        return 1 - c // 7, c % 7

    def g_copy(c, k, src, dst, peer):
        return pltpu.make_async_remote_copy(
            src_ref=src, dst_ref=dst, send_sem=gssem.at[c, k], recv_sem=grsem.at[c, k],
            device_id=peer, device_id_type=MESH)

    def core_copy(c):
        layer, j = chunk(c)
        return g_copy(c, 0, G.at[layer, ot, j], R2.at[j * H:(j + 1) * H], partner)

    def landing(c):
        layer, j = chunk(c)
        if layer == 1:
            return lambda lo, n: R2.at[7 * H + j * 192 + lo:7 * H + j * 192 + lo + n]
        return lambda lo, n: G.at[1, tp, j, lo:lo + n]

    half_p, half_q = cx * 64, 128 + cy * 64
    quarter_p, quarter_q = half_p + cy * 32, half_q + cx * 32

    def strip(c, start, n, final=False):
        layer, j = chunk(c)
        return G.at[layer, ot if final else tp, j, pl.ds(pl.multiple_of(start, 32), n)]

    def a_copies(c):
        land = landing(c)
        return [g_copy(c, 1, strip(c, 64 - half_p, 64), land(0, 64), x_peer),
                g_copy(c, 2, strip(c, 320 - half_q, 64), land(64, 64), y_peer)]

    def b_copies(c):
        land = landing(c)
        return [g_copy(c, 3, strip(c, half_p + 32 - cy * 32, 32), land(128, 32), y_peer),
                g_copy(c, 4, strip(c, half_q + 32 - cx * 32, 32), land(160, 32), x_peer)]

    def c_copies(c):
        ref_p, ref_q = strip(c, quarter_p, 32, True), strip(c, quarter_q, 32, True)
        return [g_copy(c, 5, ref_p, ref_p, y_peer), g_copy(c, 6, ref_q, ref_q, x_peer)]

    def d_copies(c):
        ref_p, ref_q = strip(c, half_p, 64, True), strip(c, half_q, 64, True)
        return [g_copy(c, 7, ref_p, ref_p, x_peer), g_copy(c, 8, ref_q, ref_q, y_peer)]

    def store_copies(c):
        layer, j = chunk(c)
        src = G.at[layer, ot, j]
        if j in (J_NW2, J_EW2):
            ref = o_nw2 if j == J_NW2 else o_ew2
            pairs = [(src.at[:, :H], ref.at[layer, :H]), (src.at[:, H:], ref.at[layer, H:])]
        elif j < J_EW2:
            pairs = [(src, o_nw1.at[layer, j - J_NW1])]
        else:
            pairs = [(src, o_ew1.at[layer, j - J_EW1])]
        return [pltpu.make_async_copy(a, b, osem.at[c, k]) for k, (a, b) in enumerate(pairs)]

    def wait_all(copies):
        for cp in copies:
            cp.wait()

    def start_all(copies):
        for cp in copies:
            cp.start()

    def stage0(c):
        core_copy(c).start()

    def stage1(c):
        layer, j = chunk(c)
        core_copy(c).wait()
        G[layer, tp, j] += R2[j * H:(j + 1) * H]
        start_all(a_copies(c))

    def stage2(c):
        land = landing(c)
        wait_all(a_copies(c))
        for start, lo in ((half_p, 0), (half_q, 64)):
            ref = strip(c, start, 64)
            ref[...] += land(lo, 64)[...]
        start_all(b_copies(c))

    def stage3(c):
        land = landing(c)
        wait_all(b_copies(c))
        for start, lo in ((quarter_p, 128), (quarter_q, 160)):
            strip(c, start, 32, True)[...] = strip(c, start, 32)[...] + land(lo, 32)[...]
        start_all(c_copies(c))

    def stage4(c):
        wait_all(c_copies(c))
        start_all(d_copies(c))

    def stage5(c):
        wait_all(d_copies(c))
        start_all(store_copies(c))

    def run(stage, chunks):
        for c in chunks:
            stage(c)

    node1, edge1, node0, edge0 = (list(range(*ends)) for ends in ((0, 3), (3, 7), (7, 10), (10, 14)))

    plan = {
        1: [(stage1, node1, 0), (stage2, node1, 4), (stage3, node1, 7)],
        0: [(stage5, node1, 0), (stage2, edge1, 1), (stage1, node0, 5), (stage3, edge1, 5), (stage4, edge1[:2], 8)],
    }

    def put_w2(layer, j, half, value, add):
        if add:
            G[layer, half, j, :, :H] += value[:H]
            G[layer, half, j, :, H:] += value[H:]
        else:
            G[layer, half, j, :, :H] = value[:H]
            G[layer, half, j, :, H:] = value[H:]

    def put_w1(layer, j, value, add):
        for half in range(2):
            if add:
                G[layer, half, j] += value[half * H:(half + 1) * H]
            else:
                G[layer, half, j] = value[half * H:(half + 1) * H]

    def mlp_bwd(d_msg, cen, hidden, gam, w2, layer, sm, j2, add):
        normed, inv_std = norm_parts(cen)
        sums = [sum_rows(d_msg * normed), sum_rows(d_msg)]
        d_normed = d_msg * gam
        d_out = inv_std * (d_normed - mean_cols(d_normed) - normed * mean_cols(d_normed * normed))
        sums = [sum_rows(d_out)] + sums
        d_out_bf = d_out.astype(BF)
        sig = gate(hidden)
        act = (hidden * sig).astype(BF)
        for half in range(2):
            put_w2(layer, j2, half, dot_rows(act, d_out_bf[:, half * H:(half + 1) * H]), add)
        d_hidden = second_t(d_out_bf, w2, layer) * (sig * (1.0 + hidden * (1.0 - sig)))
        sums = [sum_rows(d_hidden)] + sums
        for k in range(4):
            if add:
                SM[0, sm + k:sm + k + 1] += sums[k]
            else:
                SM[0, sm + k:sm + k + 1] = sums[k]
        return d_hidden.astype(BF)

    SM[...] = jnp.zeros_like(SM)

    def layer_bwd(layer, src):
        d_node = DN[...].astype(F32)
        d_hid = mlp_bwd(d_node, CN[layer], HN[layer], vec_row(layer, 1, True), W2N, layer, layer * 8, J_NW2, False)
        nodes, edge_w2, edge_w1 = (node1, edge1[:1], edge1[1:]) if layer else (node0, edge0[:1], edge0[1:])
        pl.semaphore_wait(csem.at[1 - layer], 3 if layer == 1 else 1)
        stage0(nodes[0])
        put_w1(layer, J_NW1, dot_rows(VF[layer], d_hid), False)
        stage0(nodes[1])
        put_w1(layer, J_NW1 + 1, dot_rows(SF[layer], d_hid), False)
        stage0(nodes[2])
        DV[...] = d_node + dot_cols(d_hid, full1(W1N, layer, 0))
        PS[...] = dot_cols(d_hid, full1(W1N, layer, 1)).reshape(NN, NS, D)
        for j in (J_EW2, J_EW1):
            G[layer, :, j] = jnp.zeros((2, H, D), F32)
        AG[...] = jnp.zeros_like(AG)
        PR[...] = jnp.zeros_like(PR)
        gam = vec_row(layer, 1, False)
        if layer == 0:
            for cp in fills:
                cp.wait()

        def edge(b, carry):
            for i in range(BE):
                GA[i * NS:(i + 1) * NS] = PS[rcv[b * BE + i]]
            d_edge = cat(rows_of(DE[0, edges(b)]), rows_of(DE[1, edges(b)]))
            d_hid = mlp_bwd(d_edge + GA[...], CS[erows(b)], HS[erows(b)], gam, W2E, layer, layer * 8 + 4, J_EW2, True)
            lat = cat(rows_of(src[0, edges(b)]), rows_of(src[1, edges(b)])).astype(BF)
            put_w1(layer, J_EW1, dot_rows(lat, d_hid), True)
            new = d_edge + dot_cols(d_hid, full1(W1E, layer, 0))
            DE[0, edges(b)] = new[:, :H].reshape(BE, NS, H).astype(BF)
            DE[1, edges(b)] = new[:, H:].reshape(BE, NS, H).astype(BF)
            AG[...] += dot(KS[b], d_hid)
            PR[...] += dot(KR[b], d_hid).reshape(NN, NS, D)
            for stage, chunks, first in plan[layer]:
                for i, c in enumerate(chunks):
                    pl.when(b == first + i)(functools.partial(stage, c))
            return carry

        lax.fori_loop(0, NB, edge, 0)
        if layer == 1:
            for cp in fills:
                cp.start()
        run(stage0, edge_w2 + edge_w1[:1])
        d_ps, d_pr = AG[...].astype(BF), rows_of(PR[...]).astype(BF)
        put_w1(layer, J_EW1 + 1, dot_rows(VF[layer], d_ps), False)
        stage0(edge_w1[1])
        put_w1(layer, J_EW1 + 2, dot_rows(VF[layer], d_pr), False)
        stage0(edge_w1[2])
        DN[...] = (DV[...] + dot_cols(d_ps, full1(W1E, layer, 1))
                   + dot_cols(d_pr, full1(W1E, layer, 2))).astype(BF)

    layer_bwd(1, E1)
    run(stage1, edge1)
    run(stage4, node1)
    pl.semaphore_signal(csem.at[1], inc=1, device_id=partner, device_id_type=MESH)
    layer_bwd(0, E0)
    run(stage4, edge1[2:])
    run(stage1, edge0)

    pl.semaphore_signal(csem.at[2], inc=1, device_id=partner, device_id_type=MESH)
    run(stage2, node0)
    for k, ref in ((0, VF.at[2]), (1, DN)):
        rows = ref[...].astype(F32)
        NST[2 * k] = jnp.where(tp == 0, rows[:, :H], rows[:, H:]).reshape(NN, NS, H).astype(BF)
        NF[2 * k] = jnp.where(tp == 0, rows[:, H:], rows[:, :H]).reshape(NN, NS, H)

    def out_stage(b, carry):
        HS[erows(b), :H] = rows_of(E2[ot, edges(b)])
        HS[erows(b), H:] = rows_of(DE[ot, edges(b)])
        return carry

    lax.fori_loop(0, NB, out_stage, 0)
    pl.semaphore_wait(csem.at[2], 1)
    small0 = rdma(SM.at[0], SM.at[1], 6)
    small0.start()
    node_o = [rdma(NF.at[0], NF.at[1], 4), rdma(NF.at[2], NF.at[3], 5)]
    for cp in node_o:
        cp.start()

    def out_copy(b):
        return rdma(HS.at[erows(b)], CS.at[erows(b)], 44 + b)

    for b in range(NB):
        out_copy(b).start()
    stores = [
        (E2.at[tp], o_e.at[:, mine]), (DE.at[tp], o_de.at[:, mine]),
        (NST.at[0], o_n.at[:, mine]), (NST.at[2], o_dn.at[:, mine]),
    ]
    run(stage5, edge1)
    stores = [pltpu.make_async_copy(src, dst, lsem.at[i]) for i, (src, dst) in enumerate(stores)]
    for cp in stores:
        cp.start()
    for k, cp in enumerate(node_o):
        cp.wait()
        NST[2 * k + 1] = NF[2 * k + 1].astype(BF)

    def out_recv(b, carry):
        out_copy(b).wait()
        E1[0, edges(b)] = CS[erows(b), :H].reshape(BE, NS, H).astype(BF)
        E1[1, edges(b)] = CS[erows(b), H:].reshape(BE, NS, H).astype(BF)
        return carry

    run(stage3, node0)
    lax.fori_loop(0, NB, out_recv, 0)
    more = [
        (E1.at[0], o_e.at[:, theirs]), (E1.at[1], o_de.at[:, theirs]),
        (NST.at[1], o_n.at[:, theirs]), (NST.at[3], o_dn.at[:, theirs]),
    ]
    more = [pltpu.make_async_copy(src, dst, lsem.at[6 + i]) for i, (src, dst) in enumerate(more)]
    for cp in more:
        cp.start()
    small0.wait()
    SM[2] = SM[0] + SM[1]
    small1 = pltpu.make_async_remote_copy(
        src_ref=SM.at[2], dst_ref=SM.at[3], send_sem=ssem.at[7], recv_sem=rsem.at[7],
        device_id=x_peer, device_id_type=MESH)
    small1.start()
    run(stage2, edge0)
    run(stage4, node0)
    small1.wait()
    SM[4] = SM[2] + SM[3]
    small2 = pltpu.make_async_remote_copy(
        src_ref=SM.at[4], dst_ref=SM.at[5], send_sem=ssem.at[54], recv_sem=rsem.at[54],
        device_id=y_peer, device_id_type=MESH)
    small2.start()
    run(stage3, edge0)
    small2.wait()
    total = SM[4] + SM[5]
    for layer in range(2):
        for row, ref_b, ref_v in ((0, o_bn, o_vn), (4, o_be, o_ve)):
            at = layer * 8 + row
            ref_b[layer:layer + 1] = total[at:at + 1]
            for k in range(3):
                one = total[at + 1 + k:at + 2 + k]
                ref_v[k, layer:layer + 1] = jnp.where(tp == 0, one[:, :H], one[:, H:])
    run(stage4, edge0)
    run(stage5, node0 + edge0)
    for c in node1 + edge1 + node0 + edge0:
        wait_all(store_copies(c))
    for cp in stores + more:
        cp.wait()


def compute(*args):
    any_spec = pl.BlockSpec(memory_space=pl.ANY)
    vm = pl.BlockSpec(memory_space=pltpu.VMEM)
    sm = pl.BlockSpec(memory_space=pltpu.SMEM)
    v = pltpu.VMEM
    lat = (NN, 2 * NS, H)
    edg = (NE, 2 * NS, H)
    outs = [(lat, BF), (edg, BF), (lat, BF), (edg, BF),
            ((2, 3, H, D), F32), ((2, D, H), F32), ((2, 2, H, D), F32), ((2, D, H), F32),
            ((2, D), F32), ((2, D), F32), ((3, 2, H), F32), ((3, 2, H), F32), ((2, NE * NS, D), F32)]
    dma = pltpu.SemaphoreType.DMA
    node = (ROWS, D)
    scratch = [
        v((2, 3, 2, H, D), BF), v((2, 2, D, H), BF), v((2, 2, 2, H, D), BF), v((2, 2, D, H), BF),
        *[v((2, 3, 2, H), F32)] * 2, *[v((NB, ROWS, BR), BF)] * 2, *[v((2, NE, NS, H), BF)] * 4,
        v((NE * NS, D), F32), v((NE * NS, D), F32), v((7 * (H + 192), D), F32), v((2, 2, 7, H, D), F32),
        v((NN, NS, D), F32), v((NN, NS, D), F32), v((BR, D), F32), v(node, F32),
        v((4, NN, NS, H), BF), v((4, NN, NS, H), F32),
        v((3, *node), BF), v((2, *node), BF), v((2, *node), F32), v((2, *node), F32),
        v(node, BF), v(node, F32), v((6, 16, D), F32),
        dma((12,)), dma((56,)), dma((56,)), pltpu.SemaphoreType.REGULAR((3,)), dma((4,)),
        dma((14, 9)), dma((14, 9)), dma((14, 2)),
    ]
    return pl.pallas_call(
        body,
        out_shape=[jax.ShapeDtypeStruct(*o) for o in outs],
        in_specs=[any_spec] * 8 + [vm] * 5 + [sm] * 2,
        out_specs=[any_spec] * 8 + [vm] * 4 + [any_spec],
        scratch_shapes=scratch,
        compiler_params=pltpu.CompilerParams(
            collective_id=0, has_side_effects=True, vmem_limit_bytes=67043328),
    )(*args)


def solution(mesh):
    lat_spec = P('dp', None, 'tp')
    first_spec = P(None, None, 'tp', None)
    col_spec = P(None, None, 'tp')
    param_specs = (first_spec, P(), col_spec, col_spec, first_spec, P(), col_spec, col_spec)
    in_specs = (lat_spec, lat_spec, P(), P(), lat_spec, lat_spec) + param_specs
    out_specs = (lat_spec, lat_spec, lat_spec, lat_spec) + param_specs

    def local_step(node_lat, edge_lat, senders, receivers, grad_node, grad_edge, edge_w1, edge_b1, edge_w2, edge_vec, node_w1, node_b1, node_w2, node_vec):
        def swap(x):
            return jnp.transpose(x, (1, 0, 2))

        ids = jnp.stack([senders, receivers])
        flat = ids[:, :, None] * NS + jnp.arange(NS, dtype=jnp.int32)
        outs = compute(
            swap(node_lat), swap(edge_lat), swap(grad_node), swap(grad_edge), edge_w1, edge_w2, node_w1, node_w2,
            edge_b1, node_b1, swap(edge_vec), swap(node_vec), flat.reshape(2 * NB, 1, BR), senders, receivers)
        o_ew1, o_ew2, o_nw1, o_nw2, o_be, o_bn, o_ve, o_vn = outs[4:12]
        return tuple(swap(x) for x in outs[:4]) + (o_ew1, o_be, o_ew2, swap(o_ve), o_nw1, o_bn, o_nw2, swap(o_vn))

    return jax.shard_map(local_step, mesh=mesh, in_specs=in_specs, out_specs=out_specs, check_vma=False)
```

```python
import functools

import jax
import jax.numpy as jnp
from jax import lax
from jax.experimental import pallas as pl
from jax.experimental.pallas import tpu as pltpu
from jax.sharding import PartitionSpec as P

BF = jnp.bfloat16
F32 = jnp.float32
MESH = pl.DeviceIdType.MESH
LN_EPS = 1e-5
NS = 8
NN = 42
NE = 300
D = 512
H = 256
ROWS = NN * NS
NB = 10
BE = NE // NB
BR = BE * NS


def dot(lhs, rhs, lc=1, rc=0):
    return lax.dot_general(lhs, rhs, (((lc,), (rc,)), ((), ())), preferred_element_type=F32)


def dot_rows(lhs, rhs):
    return dot(lhs, rhs, 0, 0)


def dot_cols(lhs, rhs):
    return dot(lhs, rhs, 1, 1)


def cat(lhs, rhs):
    return jnp.concatenate([lhs, rhs], axis=1)


def mean_cols(x):
    return jnp.sum(x, axis=1, keepdims=True) * (1.0 / D)


def sum_rows(x):
    return jnp.sum(x, axis=0, keepdims=True)


def norm_parts(centered):
    inv_std = lax.rsqrt(mean_cols(centered * centered) + LN_EPS)
    return centered * inv_std, inv_std


J_NW2, J_NW1, J_EW2, J_EW1 = 0, 1, 3, 4


def rows_of(block):
    return block.astype(F32).reshape(block.shape[0] * NS, block.shape[2])


def body(nl, el, gn, ge, w1e, w2e, w1n, w2n, b1e, b1n, vece, vecn, snd, rcv,
         o_n, o_e, o_dn, o_de, o_ew1, o_ew2, o_nw1, o_nw2, o_be, o_bn, o_ve, o_vn, spill,
         W1E, W2E, W1N, W2N, VE, VN, KS, KR,
         E0, E1, E2, DE, HS, CS, R2, G, PS, PR, GA, AG,
         NST, NF, VF, SF, HN, CN, DN, DV, SM,
         lsem, ssem, rsem, csem, spsem, gssem, grsem, osem):
    dp = lax.axis_index('dp')
    tp = lax.axis_index('tp')
    ot = 1 - tp
    partner = (dp, ot)
    cx, cy = lax.rem(dp, 2), dp // 2
    x_peer = (cy * 2 + 1 - cx, tp)
    y_peer = ((1 - cy) * 2 + cx, tp)
    peers = (partner, x_peer, y_peer)

    def rdma(src, dst, idx, peer=None):
        return pltpu.make_async_remote_copy(
            src_ref=src, dst_ref=dst, send_sem=ssem.at[idx], recv_sem=rsem.at[idx],
            device_id=peer or partner, device_id_type=MESH)

    def wait_all(copies):
        for cp in copies:
            cp.wait()

    def start_all(copies):
        for cp in copies:
            cp.start()

    mine = pl.ds(pl.multiple_of(tp * NS, NS), NS)
    theirs = pl.ds(pl.multiple_of(ot * NS, NS), NS)
    loads = [
        (nl.at[:, mine], NST.at[0]), (nl.at[:, theirs], NST.at[1]),
        (w1e, W1E.at[:, :, tp]), (el.at[:, theirs], E1.at[0]), (w2e, W2E.at[:, tp]),
        (el.at[:, mine], E0.at[tp]), (w1n, W1N.at[:, :, tp]), (w2n, W2N.at[:, tp]),
        (ge.at[:, theirs], E1.at[1]), (ge.at[:, mine], DE.at[tp]),
        (gn.at[:, mine], NST.at[2]), (gn.at[:, theirs], NST.at[3]),
    ]
    loads = [pltpu.make_async_copy(src, dst, lsem.at[i]) for i, (src, dst) in enumerate(loads)]
    for cp in loads:
        cp.start()

    barrier = pltpu.get_barrier_semaphore()
    for peer in peers:
        pl.semaphore_signal(barrier, inc=1, device_id=peer, device_id_type=MESH)
    loads[0].wait()
    loads[1].wait()
    NF[0] = NST[1].astype(F32)
    pl.semaphore_wait(barrier, 3)
    vec_copies = [rdma(vece, VE.at[tp], 0), rdma(vecn, VN.at[tp], 1)]
    for cp in vec_copies:
        cp.start()
    VE[tp] = vece[...]
    VN[tp] = vecn[...]

    node_x = rdma(NF.at[0], NF.at[1], 2)
    node_x.start()

    def w_pack(layer, j):
        if j == J_NW2:
            half = W2N[layer, tp]
        elif j == J_EW2:
            half = W2E[layer, tp]
        elif j < J_EW2:
            return W1N[layer, j - J_NW1, tp].astype(F32)
        else:
            return W1E[layer, j - J_EW1, tp].astype(F32)
        half = half.astype(F32)
        return cat(half[:H], half[H:])

    def w_unpack(layer, j, block):
        block = block.astype(BF)
        if j in (J_NW2, J_EW2):
            ref = W2N if j == J_NW2 else W2E
            ref[layer, ot, :H] = block[:, :H]
            ref[layer, ot, H:] = block[:, H:]
        elif j < J_EW2:
            W1N[layer, j - J_NW1, ot] = block
        else:
            W1E[layer, j - J_EW1, ot] = block

    groups = [(0, J_EW1 + 1, 2), (0, J_EW1, 1), (0, J_EW2, 1), (0, 0, 3), (1, 0, 7)]
    w_copies = [rdma(G.at[1, layer, pl.ds(lo, n)], G.at[0, layer, pl.ds(lo, n)], 8 + k)
                for k, (layer, lo, n) in enumerate(groups)]

    def w_packs(k):
        layer, lo, n = groups[k]
        for j in range(lo, lo + n):
            G[1, layer, j] = w_pack(layer, j)

    def w_recv(k):
        layer, lo, n = groups[k]
        w_copies[k].wait()
        for j in range(lo, lo + n):
            w_unpack(layer, j, G[0, layer, j])

    def edges(b):
        return pl.ds(b * BE, BE)

    def erows(b):
        return pl.ds(pl.multiple_of(b * BR, BR), BR)

    lat_copy = rdma(HS.at[:, :H], CS.at[:, :H], 6)
    grad_copy = rdma(R2.at[:NE * NS, :H], R2.at[:NE * NS, H:], 7)

    def stage_rows(dst, src):
        def one(b, carry):
            dst[erows(b), :H] = rows_of(src[edges(b)])
            return carry
        lax.fori_loop(0, NB, one, 0)

    loads[2].wait()
    for k in range(2):
        w_packs(k)
        w_copies[k].start()
    wait_all(loads[3:5])
    stage_rows(HS, E1.at[0])
    lat_copy.start()
    w_packs(2)
    w_copies[2].start()
    wait_all(loads[5:])
    w_packs(3)
    w_packs(4)
    stage_rows(R2, E1.at[1])
    NF[2] = NST[3].astype(F32)
    node_g = rdma(NF.at[2], NF.at[3], 3)

    column = lax.broadcasted_iota(jnp.int32, (NS, ROWS), 1) - lax.broadcasted_iota(jnp.int32, (NS, ROWS), 0)

    def select(dst, ids):
        def one(i, carry):
            two = [jnp.where(column == ids[2 * i + k] * NS, 1.0, 0.0) for k in range(2)]
            at = pl.ds(pl.multiple_of(i * 2 * NS, 2 * NS), 2 * NS)
            dst[at] = jnp.concatenate(two, axis=0).astype(BF)
            return carry
        lax.fori_loop(0, NE // 2, one, 0, unroll=5)

    select(KR, rcv)

    def node_in(dst, staged, received):
        own, got = rows_of(NST[staged]), rows_of(NF[received])
        lo = jnp.where(tp == 0, own, got)
        hi = jnp.where(tp == 0, got, own)
        dst[...] = cat(lo, hi).astype(BF)

    for cp in vec_copies:
        cp.wait()
    node_x.wait()
    node_in(VF.at[0], 0, 1)

    def vec_row(layer, row, node):
        ref = VN if node else VE
        return cat(ref[0, row, layer:layer + 1], ref[1, row, layer:layer + 1])

    def full1(ref, layer, k):
        return ref[layer, k].reshape(D, D)

    def gate(hidden):
        return 0.5 + 0.5 * jnp.tanh(0.5 * hidden)

    def second(act, ref, layer):
        return cat(dot(act, ref[layer, 0]), dot(act, ref[layer, 1]))

    def second_t(dout, ref, layer):
        return dot_cols(dout[:, :H], ref[layer, 0]) + dot_cols(dout[:, H:], ref[layer, 1])

    def layer_fwd(layer, src, dst):
        w_recv(0 if layer == 0 else 4)
        PS[...] = (dot(VF[layer], full1(W1E, layer, 1)) + b1e[layer:layer + 1]).reshape(NN, NS, D)
        PR[...] = dot(VF[layer], full1(W1E, layer, 2)).reshape(NN, NS, D)
        if layer == 0:
            w_recv(1)
            w_recv(2)
            lat_copy.wait()
            start_all(w_copies[3:])
        c0, gam, bet = (vec_row(layer, r, False) for r in range(3))
        AG[...] = jnp.zeros_like(AG)

        def edge(b, carry):
            if layer == 0:
                src[ot, edges(b)] = CS[erows(b), :H].reshape(BE, NS, H).astype(BF)
            for i in range(BE):
                GA[i * NS:(i + 1) * NS] = PS[snd[b * BE + i]] + PR[rcv[b * BE + i]]
            lat = cat(rows_of(src[0, edges(b)]), rows_of(src[1, edges(b)]))
            hidden = dot(lat.astype(BF), full1(W1E, layer, 0)) + GA[...]
            HS[erows(b)] = hidden
            act = (hidden * gate(hidden)).astype(BF)
            out = second(act, W2E, layer) + c0
            cen = out - mean_cols(out)
            CS[erows(b)] = cen
            normed, unused = norm_parts(cen)
            msg = (normed * gam + bet).astype(BF)
            AG[...] += dot_rows(KR[erows(b)], msg)
            new = lat + msg.astype(F32)
            dst[0, edges(b)] = new[:, :H].reshape(BE, NS, H).astype(BF)
            dst[1, edges(b)] = new[:, H:].reshape(BE, NS, H).astype(BF)
            return carry

        lax.fori_loop(0, NB, edge, 0)
        if layer == 0:
            start_all(spills)
            start_all([grad_copy, node_g])
            w_recv(3)
        SF[layer] = AG[...].astype(BF)
        lat = VF[layer]
        hidden = dot(lat, full1(W1N, layer, 0)) + dot(SF[layer], full1(W1N, layer, 1)) + b1n[layer:layer + 1]
        HN[layer] = hidden
        act = (hidden * gate(hidden)).astype(BF)
        out = second(act, W2N, layer) + vec_row(layer, 0, True)
        cen = out - mean_cols(out)
        CN[layer] = cen
        normed, unused = norm_parts(cen)
        msg = (normed * vec_row(layer, 1, True) + vec_row(layer, 2, True)).astype(BF)
        VF[layer + 1] = (lat.astype(F32) + msg.astype(F32)).astype(BF)

    spills = [pltpu.make_async_copy(HS, spill.at[0], spsem.at[0]), pltpu.make_async_copy(CS, spill.at[1], spsem.at[1])]
    fills = [pltpu.make_async_copy(spill.at[0], HS, spsem.at[2]), pltpu.make_async_copy(spill.at[1], CS, spsem.at[3])]

    layer_fwd(0, E0, E1)
    select(KS, snd)
    wait_all(spills)
    layer_fwd(1, E1, E2)
    grad_copy.wait()

    def grad_rows(b, carry):
        DE[ot, edges(b)] = R2[erows(b), H:].reshape(BE, NS, H).astype(BF)
        return carry

    lax.fori_loop(0, NB, grad_rows, 0)
    for peer in peers:
        pl.semaphore_signal(csem.at[0], inc=1, device_id=peer, device_id_type=MESH)
    node_g.wait()
    node_in(DN, 2, 3)

    def chunk(c):
        return 1 - c // 7, c % 7

    def g_copy(c, send, k, src, dst, peer):
        return pltpu.make_async_remote_copy(
            src_ref=src, dst_ref=dst, send_sem=gssem.at[c % 7, send], recv_sem=grsem.at[c % 7, k],
            device_id=peer, device_id_type=MESH)

    def core_copy(c):
        layer, j = chunk(c)
        return g_copy(c, 0, 0, G.at[layer, ot, j], R2.at[j * H:(j + 1) * H], partner)

    def landing(c):
        layer, j = chunk(c)
        if layer == 1:
            return lambda lo, n: R2.at[7 * H + j * 192 + lo:7 * H + j * 192 + lo + n]
        return lambda lo, n: G.at[1, tp, j, lo:lo + n]

    half_p, half_q = cx * 64, 128 + cy * 64
    quarter_p, quarter_q = half_p + cy * 32, half_q + cx * 32

    def strip(c, start, n, final=False):
        layer, j = chunk(c)
        return G.at[layer, ot if final else tp, j, pl.ds(pl.multiple_of(start, 32), n)]

    def a_copies(c):
        land = landing(c)
        return [g_copy(c, 1, 1, strip(c, 64 - half_p, 64), land(0, 64), x_peer),
                g_copy(c, 2, 2, strip(c, 320 - half_q, 64), land(64, 64), y_peer)]

    def b_copies(c):
        land = landing(c)
        return [g_copy(c, 1, 3, strip(c, half_p + 32 - cy * 32, 32), land(128, 32), y_peer),
                g_copy(c, 2, 4, strip(c, half_q + 32 - cx * 32, 32), land(160, 32), x_peer)]

    def c_copies(c):
        ref_p, ref_q = strip(c, quarter_p, 32, True), strip(c, quarter_q, 32, True)
        return [g_copy(c, 1, 5, ref_p, ref_p, y_peer), g_copy(c, 2, 6, ref_q, ref_q, x_peer)]

    def d_copies(c):
        ref_p, ref_q = strip(c, half_p, 64, True), strip(c, half_q, 64, True)
        return [g_copy(c, 1, 7, ref_p, ref_p, x_peer), g_copy(c, 2, 8, ref_q, ref_q, y_peer)]

    def store_copies(c):
        layer, j = chunk(c)
        src = G.at[layer, ot, j]
        if j in (J_NW2, J_EW2):
            ref = o_nw2 if j == J_NW2 else o_ew2
            pairs = [(src.at[:, :H], ref.at[layer, :H]), (src.at[:, H:], ref.at[layer, H:])]
        elif j < J_EW2:
            pairs = [(src, o_nw1.at[layer, j - J_NW1])]
        else:
            pairs = [(src, o_ew1.at[layer, j - J_EW1])]
        return [pltpu.make_async_copy(a, b, osem.at[c % 7, k]) for k, (a, b) in enumerate(pairs)]

    def stage0(c):
        core_copy(c).start()

    def stage1(c):
        layer, j = chunk(c)
        core_copy(c).wait()
        G[layer, tp, j] += R2[j * H:(j + 1) * H]
        start_all(a_copies(c))

    def stage2(c):
        land = landing(c)
        wait_all(a_copies(c))
        for start, lo in ((half_p, 0), (half_q, 64)):
            ref = strip(c, start, 64)
            ref[...] += land(lo, 64)[...]
        start_all(b_copies(c))

    def stage3(c):
        land = landing(c)
        wait_all(b_copies(c))
        for start, lo in ((quarter_p, 128), (quarter_q, 160)):
            strip(c, start, 32, True)[...] = strip(c, start, 32)[...] + land(lo, 32)[...]
        start_all(c_copies(c))

    def stage4(c):
        wait_all(c_copies(c))
        start_all(d_copies(c))

    def stage5(c):
        wait_all(d_copies(c))
        if c >= 7:
            wait_all(store_copies(c - 7))
        start_all(store_copies(c))

    def run(stage, chunks):
        for c in chunks:
            stage(c)

    node1, edge1, node0, edge0 = (list(range(*ends)) for ends in ((0, 3), (3, 7), (7, 10), (10, 14)))

    plan = {
        1: [(stage1, node1, 0), (stage2, node1, 4), (stage3, node1, 7)],
        0: [(stage5, node1, 0), (stage2, edge1, 1), (stage1, node0, 5), (stage3, edge1, 5), (stage4, edge1[:2], 8)],
    }

    def put_w2(layer, j, half, value, add):
        if add:
            G[layer, half, j, :, :H] += value[:H]
            G[layer, half, j, :, H:] += value[H:]
        else:
            G[layer, half, j, :, :H] = value[:H]
            G[layer, half, j, :, H:] = value[H:]

    def put_w1(layer, j, value, add=False):
        for half in range(2):
            if add:
                G[layer, half, j] += value[half * H:(half + 1) * H]
            else:
                G[layer, half, j] = value[half * H:(half + 1) * H]

    def mlp_bwd(d_msg, cen, hidden, gam, w2, layer, sm, j2, add):
        normed, inv_std = norm_parts(cen)
        sums = [sum_rows(d_msg * normed), sum_rows(d_msg)]
        d_normed = d_msg * gam
        d_out = inv_std * (d_normed - mean_cols(d_normed) - normed * mean_cols(d_normed * normed))
        sums = [sum_rows(d_out)] + sums
        d_out_bf = d_out.astype(BF)
        sig = gate(hidden)
        act = (hidden * sig).astype(BF)
        for half in range(2):
            put_w2(layer, j2, half, dot_rows(act, d_out_bf[:, half * H:(half + 1) * H]), add)
        d_hidden = second_t(d_out_bf, w2, layer) * (sig * (1.0 + hidden * (1.0 - sig)))
        sums = [sum_rows(d_hidden)] + sums
        for k in range(4):
            if add:
                SM[0, sm + k:sm + k + 1] += sums[k]
            else:
                SM[0, sm + k:sm + k + 1] = sums[k]
        return d_hidden.astype(BF)

    SM[...] = jnp.zeros_like(SM)

    def layer_bwd(layer, src):
        d_node = DN[...].astype(F32)
        d_hid = mlp_bwd(d_node, CN[layer], HN[layer], vec_row(layer, 1, True), W2N, layer, layer * 8, J_NW2, False)
        nodes, edge_w2, edge_w1 = (node1, edge1[:1], edge1[1:]) if layer else (node0, edge0[:1], edge0[1:])
        pl.semaphore_wait(csem.at[1 - layer], 3 if layer == 1 else 1)
        stage0(nodes[0])
        put_w1(layer, J_NW1, dot_rows(VF[layer], d_hid))
        stage0(nodes[1])
        put_w1(layer, J_NW1 + 1, dot_rows(SF[layer], d_hid))
        stage0(nodes[2])
        DV[...] = d_node + dot_cols(d_hid, full1(W1N, layer, 0))
        PS[...] = dot_cols(d_hid, full1(W1N, layer, 1)).reshape(NN, NS, D)
        for j in (J_EW2, J_EW1):
            G[layer, :, j] = jnp.zeros((2, H, D), F32)
        AG[...] = jnp.zeros_like(AG)
        PR[...] = jnp.zeros_like(PR)
        gam = vec_row(layer, 1, False)
        if layer == 0:
            for cp in fills:
                cp.wait()

        def edge(b, carry):
            for i in range(BE):
                GA[i * NS:(i + 1) * NS] = PS[rcv[b * BE + i]]
            d_edge = cat(rows_of(DE[0, edges(b)]), rows_of(DE[1, edges(b)]))
            d_hid = mlp_bwd(d_edge + GA[...], CS[erows(b)], HS[erows(b)], gam, W2E, layer, layer * 8 + 4, J_EW2, True)
            lat = cat(rows_of(src[0, edges(b)]), rows_of(src[1, edges(b)])).astype(BF)
            put_w1(layer, J_EW1, dot_rows(lat, d_hid), True)
            new = d_edge + dot_cols(d_hid, full1(W1E, layer, 0))
            DE[0, edges(b)] = new[:, :H].reshape(BE, NS, H).astype(BF)
            DE[1, edges(b)] = new[:, H:].reshape(BE, NS, H).astype(BF)
            AG[...] += dot_rows(KS[erows(b)], d_hid)
            PR[...] += dot_rows(KR[erows(b)], d_hid).reshape(NN, NS, D)
            for stage, chunks, first in plan[layer]:
                for i, c in enumerate(chunks):
                    pl.when(b == first + i)(functools.partial(stage, c))
            return carry

        lax.fori_loop(0, NB, edge, 0)
        if layer == 1:
            for cp in fills:
                cp.start()
        run(stage0, edge_w2 + edge_w1[:1])
        d_ps, d_pr = AG[...].astype(BF), rows_of(PR[...]).astype(BF)
        put_w1(layer, J_EW1 + 1, dot_rows(VF[layer], d_ps))
        stage0(edge_w1[1])
        put_w1(layer, J_EW1 + 2, dot_rows(VF[layer], d_pr))
        stage0(edge_w1[2])
        DN[...] = (DV[...] + dot_cols(d_ps, full1(W1E, layer, 1))
                   + dot_cols(d_pr, full1(W1E, layer, 2))).astype(BF)

    layer_bwd(1, E1)
    run(stage1, edge1)
    run(stage4, node1)
    pl.semaphore_signal(csem.at[1], inc=1, device_id=partner, device_id_type=MESH)
    layer_bwd(0, E0)
    run(stage4, edge1[2:])
    run(stage1, edge0)

    pl.semaphore_signal(csem.at[2], inc=1, device_id=partner, device_id_type=MESH)
    run(stage2, node0)
    for k, ref in ((0, VF.at[2]), (1, DN)):
        rows = ref[...].astype(F32)
        NST[2 * k] = jnp.where(tp == 0, rows[:, :H], rows[:, H:]).reshape(NN, NS, H).astype(BF)
        NF[2 * k] = jnp.where(tp == 0, rows[:, H:], rows[:, :H]).reshape(NN, NS, H)

    def out_stage(b, carry):
        HS[erows(b), :H] = rows_of(E2[ot, edges(b)])
        HS[erows(b), H:] = rows_of(DE[ot, edges(b)])
        return carry

    lax.fori_loop(0, NB, out_stage, 0)
    pl.semaphore_wait(csem.at[2], 1)
    small0 = rdma(SM.at[0], SM.at[1], 2)
    small0.start()
    node_o = [rdma(NF.at[0], NF.at[1], 4), rdma(NF.at[2], NF.at[3], 5)]
    for cp in node_o:
        cp.start()

    out_copy = rdma(HS, CS, 6)
    out_copy.start()
    stores = [
        (E2.at[tp], o_e.at[:, mine]), (DE.at[tp], o_de.at[:, mine]),
        (NST.at[0], o_n.at[:, mine]), (NST.at[2], o_dn.at[:, mine]),
    ]
    run(stage5, edge1)
    stores = [pltpu.make_async_copy(src, dst, lsem.at[i]) for i, (src, dst) in enumerate(stores)]
    for cp in stores:
        cp.start()
    for k, cp in enumerate(node_o):
        cp.wait()
        NST[2 * k + 1] = NF[2 * k + 1].astype(BF)

    def out_recv(b, carry):
        E1[0, edges(b)] = CS[erows(b), :H].reshape(BE, NS, H).astype(BF)
        E1[1, edges(b)] = CS[erows(b), H:].reshape(BE, NS, H).astype(BF)
        return carry

    run(stage3, node0)
    out_copy.wait()
    lax.fori_loop(0, NB, out_recv, 0)
    more = [
        (E1.at[0], o_e.at[:, theirs]), (E1.at[1], o_de.at[:, theirs]),
        (NST.at[1], o_n.at[:, theirs]), (NST.at[3], o_dn.at[:, theirs]),
    ]
    more = [pltpu.make_async_copy(src, dst, lsem.at[6 + i]) for i, (src, dst) in enumerate(more)]
    for cp in more:
        cp.start()
    small0.wait()
    SM[2] = SM[0] + SM[1]
    small1 = rdma(SM.at[2], SM.at[3], 3, x_peer)
    small1.start()
    run(stage2, edge0)
    run(stage4, node0)
    small1.wait()
    SM[4] = SM[2] + SM[3]
    small2 = rdma(SM.at[4], SM.at[5], 13, y_peer)
    small2.start()
    run(stage3, edge0)
    small2.wait()
    total = SM[4] + SM[5]
    for layer in range(2):
        for row, ref_b, ref_v in ((0, o_bn, o_vn), (4, o_be, o_ve)):
            at = layer * 8 + row
            ref_b[layer:layer + 1] = total[at:at + 1]
            for k in range(3):
                one = total[at + 1 + k:at + 2 + k]
                ref_v[k, layer:layer + 1] = jnp.where(tp == 0, one[:, :H], one[:, H:])
    run(stage4, edge0)
    run(stage5, node0 + edge0)
    for c in node0 + edge0:
        wait_all(store_copies(c))
    for cp in stores + more:
        cp.wait()


def compute(*args):
    any_spec = pl.BlockSpec(memory_space=pl.ANY)
    vm = pl.BlockSpec(memory_space=pltpu.VMEM)
    sm = pl.BlockSpec(memory_space=pltpu.SMEM)
    v = pltpu.VMEM
    lat = (NN, 2 * NS, H)
    edg = (NE, 2 * NS, H)
    outs = [(lat, BF), (edg, BF), (lat, BF), (edg, BF),
            ((2, 3, H, D), F32), ((2, D, H), F32), ((2, 2, H, D), F32), ((2, D, H), F32),
            ((2, D), F32), ((2, D), F32), ((3, 2, H), F32), ((3, 2, H), F32), ((2, NE * NS, D), F32)]
    dma = pltpu.SemaphoreType.DMA
    node = (ROWS, D)
    scratch = [
        v((2, 3, 2, H, D), BF), v((2, 2, D, H), BF), v((2, 2, 2, H, D), BF), v((2, 2, D, H), BF),
        *[v((2, 3, 2, H), F32)] * 2, *[v((NE * NS, ROWS), BF)] * 2, *[v((2, NE, NS, H), BF)] * 4,
        v((NE * NS, D), F32), v((NE * NS, D), F32), v((7 * (H + 192), D), F32), v((2, 2, 7, H, D), F32),
        v((NN, NS, D), F32), v((NN, NS, D), F32), v((BR, D), F32), v(node, F32),
        v((4, NN, NS, H), BF), v((4, NN, NS, H), F32),
        v((3, *node), BF), v((2, *node), BF), v((2, *node), F32), v((2, *node), F32),
        v(node, BF), v(node, F32), v((6, 16, D), F32),
        dma((12,)), dma((14,)), dma((14,)), pltpu.SemaphoreType.REGULAR((3,)), dma((4,)),
        dma((7, 3)), dma((7, 9)), dma((7, 2)),
    ]
    return pl.pallas_call(
        body,
        out_shape=[jax.ShapeDtypeStruct(*o) for o in outs],
        in_specs=[any_spec] * 8 + [vm] * 4 + [sm] * 2,
        out_specs=[any_spec] * 8 + [vm] * 4 + [any_spec],
        scratch_shapes=scratch,
        compiler_params=pltpu.CompilerParams(
            collective_id=0, has_side_effects=True, vmem_limit_bytes=67043328),
    )(*args)


def mover(*refs):
    n = (len(refs) - 2) // 3
    pieces = []
    for src, dst, buf in zip(refs[:n], refs[n:2 * n], refs[2 * n:]):
        step = -(-src.shape[0] // (4 if src.size > 1 << 18 else 1))
        for lo in range(0, src.shape[0], step):
            at = pl.ds(lo, min(step, src.shape[0] - lo))
            k = len(pieces)
            pieces.append((pltpu.make_async_copy(src.at[at], buf.at[at], refs[-2].at[k]),
                           pltpu.make_async_copy(buf.at[at], dst.at[at], refs[-1].at[k])))
    for get, unused in pieces:
        get.start()
    for get, put in pieces:
        get.wait()
        put.start()
    for unused, put in pieces:
        put.wait()


def move(arrays):
    any_spec = pl.BlockSpec(memory_space=pl.ANY)
    shapes = [jax.ShapeDtypeStruct(x.shape, x.dtype) for x in arrays]
    return pl.pallas_call(
        mover, out_shape=shapes, in_specs=[any_spec] * len(arrays), out_specs=[any_spec] * len(arrays),
        scratch_shapes=[pltpu.VMEM(x.shape, x.dtype) for x in arrays] + [pltpu.SemaphoreType.DMA((24,))] * 2,
        compiler_params=pltpu.CompilerParams(vmem_limit_bytes=67043328))(*arrays)


def solution(mesh):
    lat_spec = P('dp', None, 'tp')
    first_spec = P(None, None, 'tp', None)
    col_spec = P(None, None, 'tp')
    param_specs = (first_spec, P(), col_spec, col_spec, first_spec, P(), col_spec, col_spec)
    in_specs = (lat_spec, lat_spec, P(), P(), lat_spec, lat_spec) + param_specs
    out_specs = (lat_spec, lat_spec, lat_spec, lat_spec) + param_specs

    def local_step(node_lat, edge_lat, senders, receivers, grad_node, grad_edge, edge_w1, edge_b1, edge_w2, edge_vec, node_w1, node_b1, node_w2, node_vec):
        def swap(x):
            return jnp.transpose(x, (1, 0, 2))

        outs = compute(
            swap(node_lat), swap(edge_lat), swap(grad_node), swap(grad_edge), edge_w1, edge_w2, node_w1, node_w2,
            edge_b1, node_b1, swap(edge_vec), swap(node_vec), senders, receivers)
        outs = move(outs[:12])
        o_ew1, o_ew2, o_nw1, o_nw2, o_be, o_bn, o_ve, o_vn = outs[4:]
        return tuple(swap(x) for x in outs[:4]) + (o_ew1, o_be, o_ew2, swap(o_ve), o_nw1, o_bn, o_nw2, swap(o_vn))

    return jax.shard_map(local_step, mesh=mesh, in_specs=in_specs, out_specs=out_specs, check_vma=False)
```

```python
import functools

import jax
import jax.numpy as jnp
from jax import lax
from jax.experimental import pallas as pl
from jax.experimental.pallas import tpu as pltpu
from jax.sharding import PartitionSpec as P

BF = jnp.bfloat16
F32 = jnp.float32
MESH = pl.DeviceIdType.MESH
LN_EPS = 1e-5
NS = 8
NN = 42
NE = 300
D = 512
H = 256
ROWS = NN * NS
NB = 10
BE = NE // NB
WIDE = 60


def dot(lhs, rhs, lc=1, rc=0):
    return lax.dot_general(lhs, rhs, (((lc,), (rc,)), ((), ())), preferred_element_type=F32)


def dot_rows(lhs, rhs):
    return dot(lhs, rhs, 0, 0)


def dot_cols(lhs, rhs):
    return dot(lhs, rhs, 1, 1)


def cat(lhs, rhs):
    return jnp.concatenate([lhs, rhs], axis=1)


def mean_cols(x):
    return jnp.sum(x, axis=1, keepdims=True) * (1.0 / D)


def sum_rows(x):
    return jnp.sum(x, axis=0, keepdims=True)


def norm_parts(centered):
    inv_std = lax.rsqrt(mean_cols(centered * centered) + LN_EPS)
    return centered * inv_std, inv_std


J_NW2, J_NW1, J_EW2, J_EW1 = 0, 1, 3, 4


def rows_of(block):
    return block.astype(F32).reshape(block.shape[0] * NS, block.shape[2])


def body(nl, el, gn, ge, w1e, w2e, w1n, w2n, b1e, b1n, vece, vecn, snd, rcv,
         o_n, o_e, o_dn, o_de, o_ew1, o_ew2, o_nw1, o_nw2, o_be, o_bn, o_ve, o_vn, spill,
         W1E, W2E, W1N, W2N, VE, VN, KS, KR,
         E0, E1, E2, DE, HS, CS, R2, G, PS, PR, GA, AG,
         NST, NF, VF, SF, HN, CN, DN, DV, SM,
         lsem, ssem, rsem, csem, spsem, gssem, grsem, osem):
    dp = lax.axis_index('dp')
    tp = lax.axis_index('tp')
    ot = 1 - tp
    partner = (dp, ot)
    cx, cy = lax.rem(dp, 2), dp // 2
    x_peer = (cy * 2 + 1 - cx, tp)
    y_peer = ((1 - cy) * 2 + cx, tp)
    peers = (partner, x_peer, y_peer)

    def rdma(src, dst, idx, peer=None):
        return pltpu.make_async_remote_copy(
            src_ref=src, dst_ref=dst, send_sem=ssem.at[idx], recv_sem=rsem.at[idx],
            device_id=peer or partner, device_id_type=MESH)

    def wait_all(copies):
        for cp in copies:
            cp.wait()

    def start_all(copies):
        for cp in copies:
            cp.start()

    mine = pl.ds(pl.multiple_of(tp * NS, NS), NS)
    theirs = pl.ds(pl.multiple_of(ot * NS, NS), NS)
    loads = [
        (nl.at[:, mine], NST.at[0]), (nl.at[:, theirs], NST.at[1]),
        (w1e, W1E.at[:, :, tp]), (el.at[:, theirs], E1.at[0]), (w2e, W2E.at[:, tp]),
        (el.at[:, mine], E0.at[tp]), (w1n, W1N.at[:, :, tp]), (w2n, W2N.at[:, tp]),
        (ge.at[:, theirs], E1.at[1]), (ge.at[:, mine], DE.at[tp]),
        (gn.at[:, mine], NST.at[2]), (gn.at[:, theirs], NST.at[3]),
    ]
    loads = [pltpu.make_async_copy(src, dst, lsem.at[i]) for i, (src, dst) in enumerate(loads)]
    for cp in loads:
        cp.start()

    barrier = pltpu.get_barrier_semaphore()
    for peer in peers:
        pl.semaphore_signal(barrier, inc=1, device_id=peer, device_id_type=MESH)
    loads[0].wait()
    loads[1].wait()
    NF[0] = NST[1].astype(F32)
    pl.semaphore_wait(barrier, 3)
    vec_copies = [rdma(vece, VE.at[tp], 0), rdma(vecn, VN.at[tp], 1)]
    for cp in vec_copies:
        cp.start()
    VE[tp] = vece[...]
    VN[tp] = vecn[...]

    node_x = rdma(NF.at[0], NF.at[1], 2)
    node_x.start()

    def w_pack(layer, j):
        if j == J_NW2:
            half = W2N[layer, tp]
        elif j == J_EW2:
            half = W2E[layer, tp]
        elif j < J_EW2:
            return W1N[layer, j - J_NW1, tp].astype(F32)
        else:
            return W1E[layer, j - J_EW1, tp].astype(F32)
        half = half.astype(F32)
        return cat(half[:H], half[H:])

    def w_unpack(layer, j, block):
        block = block.astype(BF)
        if j in (J_NW2, J_EW2):
            ref = W2N if j == J_NW2 else W2E
            ref[layer, ot, :H] = block[:, :H]
            ref[layer, ot, H:] = block[:, H:]
        elif j < J_EW2:
            W1N[layer, j - J_NW1, ot] = block
        else:
            W1E[layer, j - J_EW1, ot] = block

    groups = [(0, J_EW1 + 1, 2), (0, J_EW1, 1), (0, J_EW2, 1), (0, 0, 3), (1, 0, 7)]
    w_copies = [rdma(G.at[1, layer, pl.ds(lo, n)], G.at[0, layer, pl.ds(lo, n)], 8 + k)
                for k, (layer, lo, n) in enumerate(groups)]

    def w_packs(k):
        layer, lo, n = groups[k]
        for j in range(lo, lo + n):
            G[1, layer, j] = w_pack(layer, j)

    def w_recv(k):
        layer, lo, n = groups[k]
        w_copies[k].wait()
        for j in range(lo, lo + n):
            w_unpack(layer, j, G[0, layer, j])

    def edges(b, n=BE):
        return pl.ds(b * n, n)

    def erows(b, n=BE):
        return pl.ds(pl.multiple_of(b * n * NS, n * NS), n * NS)

    lat_copy = rdma(HS.at[:, :H], CS.at[:, :H], 6)
    grad_copy = rdma(R2.at[:NE * NS, :H], R2.at[:NE * NS, H:], 7)

    def stage_rows(dst, src):
        def one(b, carry):
            dst[erows(b), :H] = rows_of(src[edges(b)])
            return carry
        lax.fori_loop(0, NB, one, 0)

    loads[2].wait()
    for k in range(2):
        w_packs(k)
        w_copies[k].start()
    wait_all(loads[3:5])
    stage_rows(HS, E1.at[0])
    lat_copy.start()
    w_packs(2)
    w_copies[2].start()
    wait_all(loads[5:])
    w_packs(3)
    w_packs(4)
    stage_rows(R2, E1.at[1])
    NF[2] = NST[3].astype(F32)
    node_g = rdma(NF.at[2], NF.at[3], 3)

    column = lax.broadcasted_iota(jnp.int32, (NS, ROWS), 1) - lax.broadcasted_iota(jnp.int32, (NS, ROWS), 0)

    def select(dst, ids):
        def one(i, carry):
            two = [jnp.where(column == ids[2 * i + k] * NS, 1.0, 0.0) for k in range(2)]
            at = pl.ds(pl.multiple_of(i * 2 * NS, 2 * NS), 2 * NS)
            dst[at] = jnp.concatenate(two, axis=0).astype(BF)
            return carry
        lax.fori_loop(0, NE // 2, one, 0, unroll=5)

    select(KR, rcv)

    def node_in(dst, staged, received):
        own, got = rows_of(NST[staged]), rows_of(NF[received])
        lo = jnp.where(tp == 0, own, got)
        hi = jnp.where(tp == 0, got, own)
        dst[...] = cat(lo, hi).astype(BF)

    for cp in vec_copies:
        cp.wait()
    node_x.wait()
    node_in(VF.at[0], 0, 1)

    def vec_row(layer, row, node):
        ref = VN if node else VE
        return cat(ref[0, row, layer:layer + 1], ref[1, row, layer:layer + 1])

    def full1(ref, layer, k):
        return ref[layer, k].reshape(D, D)

    def gate(hidden):
        return 0.5 + 0.5 * jnp.tanh(0.5 * hidden)

    def second(act, ref, layer):
        return cat(dot(act, ref[layer, 0]), dot(act, ref[layer, 1]))

    def second_t(dout, ref, layer):
        return dot_cols(dout[:, :H], ref[layer, 0]) + dot_cols(dout[:, H:], ref[layer, 1])

    def layer_fwd(layer, src, dst):
        w_recv(0 if layer == 0 else 4)
        PS[...] = (dot(VF[layer], full1(W1E, layer, 1)) + b1e[layer:layer + 1]).reshape(NN, NS, D)
        PR[...] = dot(VF[layer], full1(W1E, layer, 2)).reshape(NN, NS, D)
        if layer == 0:
            w_recv(1)
            w_recv(2)
            lat_copy.wait()
            start_all(w_copies[3:])
        c0, gam, bet = (vec_row(layer, r, False) for r in range(3))
        AG[...] = jnp.zeros_like(AG)

        def edge(b, carry):
            if layer == 0:
                src[ot, edges(b, WIDE)] = CS[erows(b, WIDE), :H].reshape(WIDE, NS, H).astype(BF)
            for i in range(WIDE):
                GA[i * NS:(i + 1) * NS] = PS[snd[b * WIDE + i]] + PR[rcv[b * WIDE + i]]
            lat = cat(rows_of(src[0, edges(b, WIDE)]), rows_of(src[1, edges(b, WIDE)]))
            hidden = dot(lat.astype(BF), full1(W1E, layer, 0)) + GA[...]
            HS[erows(b, WIDE)] = hidden
            act = (hidden * gate(hidden)).astype(BF)
            out = second(act, W2E, layer) + c0
            cen = out - mean_cols(out)
            CS[erows(b, WIDE)] = cen
            normed, unused = norm_parts(cen)
            msg = (normed * gam + bet).astype(BF)
            AG[...] += dot_rows(KR[erows(b, WIDE)], msg)
            new = lat + msg.astype(F32)
            dst[0, edges(b, WIDE)] = new[:, :H].reshape(WIDE, NS, H).astype(BF)
            dst[1, edges(b, WIDE)] = new[:, H:].reshape(WIDE, NS, H).astype(BF)
            return carry

        lax.fori_loop(0, NE // WIDE, edge, 0)
        if layer == 0:
            start_all(spills)
            start_all([grad_copy, node_g])
            w_recv(3)
        SF[layer] = AG[...].astype(BF)
        lat = VF[layer]
        hidden = dot(lat, full1(W1N, layer, 0)) + dot(SF[layer], full1(W1N, layer, 1)) + b1n[layer:layer + 1]
        HN[layer] = hidden
        act = (hidden * gate(hidden)).astype(BF)
        out = second(act, W2N, layer) + vec_row(layer, 0, True)
        cen = out - mean_cols(out)
        CN[layer] = cen
        normed, unused = norm_parts(cen)
        msg = (normed * vec_row(layer, 1, True) + vec_row(layer, 2, True)).astype(BF)
        VF[layer + 1] = (lat.astype(F32) + msg.astype(F32)).astype(BF)

    spills = [pltpu.make_async_copy(HS, spill.at[0], spsem.at[0]), pltpu.make_async_copy(CS, spill.at[1], spsem.at[1])]
    fills = [pltpu.make_async_copy(spill.at[0], HS, spsem.at[2]), pltpu.make_async_copy(spill.at[1], CS, spsem.at[3])]

    layer_fwd(0, E0, E1)
    select(KS, snd)
    wait_all(spills)
    layer_fwd(1, E1, E2)
    grad_copy.wait()

    def grad_rows(b, carry):
        DE[ot, edges(b)] = R2[erows(b), H:].reshape(BE, NS, H).astype(BF)
        return carry

    lax.fori_loop(0, NB, grad_rows, 0)
    for peer in peers:
        pl.semaphore_signal(csem.at[0], inc=1, device_id=peer, device_id_type=MESH)
    node_g.wait()
    node_in(DN, 2, 3)

    def chunk(c):
        return 1 - c // 7, c % 7

    def g_copy(c, send, k, src, dst, peer):
        return pltpu.make_async_remote_copy(
            src_ref=src, dst_ref=dst, send_sem=gssem.at[c % 7, send], recv_sem=grsem.at[c % 7, k],
            device_id=peer, device_id_type=MESH)

    def core_copy(c):
        layer, j = chunk(c)
        return g_copy(c, 0, 0, G.at[layer, ot, j], R2.at[j * H:(j + 1) * H], partner)

    def landing(c):
        layer, j = chunk(c)
        if layer == 1:
            return lambda lo, n: R2.at[7 * H + j * 192 + lo:7 * H + j * 192 + lo + n]
        return lambda lo, n: G.at[1, tp, j, lo:lo + n]

    half_p, half_q = cx * 64, 128 + cy * 64
    quarter_p, quarter_q = half_p + cy * 32, half_q + cx * 32

    def strip(c, start, n, final=False):
        layer, j = chunk(c)
        return G.at[layer, ot if final else tp, j, pl.ds(pl.multiple_of(start, 32), n)]

    def a_copies(c):
        land = landing(c)
        return [g_copy(c, 1, 1, strip(c, 64 - half_p, 64), land(0, 64), x_peer),
                g_copy(c, 2, 2, strip(c, 320 - half_q, 64), land(64, 64), y_peer)]

    def b_copies(c):
        land = landing(c)
        return [g_copy(c, 1, 3, strip(c, half_p + 32 - cy * 32, 32), land(128, 32), y_peer),
                g_copy(c, 2, 4, strip(c, half_q + 32 - cx * 32, 32), land(160, 32), x_peer)]

    def c_copies(c):
        ref_p, ref_q = strip(c, quarter_p, 32, True), strip(c, quarter_q, 32, True)
        return [g_copy(c, 1, 5, ref_p, ref_p, y_peer), g_copy(c, 2, 6, ref_q, ref_q, x_peer)]

    def d_copies(c):
        ref_p, ref_q = strip(c, half_p, 64, True), strip(c, half_q, 64, True)
        return [g_copy(c, 1, 7, ref_p, ref_p, x_peer), g_copy(c, 2, 8, ref_q, ref_q, y_peer)]

    def store_copies(c):
        layer, j = chunk(c)
        src = G.at[layer, ot, j]
        if j in (J_NW2, J_EW2):
            ref = o_nw2 if j == J_NW2 else o_ew2
            pairs = [(src.at[:, :H], ref.at[layer, :H]), (src.at[:, H:], ref.at[layer, H:])]
        elif j < J_EW2:
            pairs = [(src, o_nw1.at[layer, j - J_NW1])]
        else:
            pairs = [(src, o_ew1.at[layer, j - J_EW1])]
        return [pltpu.make_async_copy(a, b, osem.at[c % 7, k]) for k, (a, b) in enumerate(pairs)]

    def stage0(c):
        core_copy(c).start()

    def stage1(c):
        layer, j = chunk(c)
        core_copy(c).wait()
        G[layer, tp, j] += R2[j * H:(j + 1) * H]
        start_all(a_copies(c))

    def stage2(c):
        land = landing(c)
        wait_all(a_copies(c))
        for start, lo in ((half_p, 0), (half_q, 64)):
            ref = strip(c, start, 64)
            ref[...] += land(lo, 64)[...]
        start_all(b_copies(c))

    def stage3(c):
        land = landing(c)
        wait_all(b_copies(c))
        for start, lo in ((quarter_p, 128), (quarter_q, 160)):
            strip(c, start, 32, True)[...] = strip(c, start, 32)[...] + land(lo, 32)[...]
        start_all(c_copies(c))

    def stage4(c):
        wait_all(c_copies(c))
        start_all(d_copies(c))

    def stage5(c):
        wait_all(d_copies(c))
        if c >= 7:
            wait_all(store_copies(c - 7))
        start_all(store_copies(c))

    def run(stage, chunks):
        for c in chunks:
            stage(c)

    node1, edge1, node0, edge0 = (list(range(*ends)) for ends in ((0, 3), (3, 7), (7, 10), (10, 14)))

    plan = {
        1: [(stage1, node1, 0), (stage2, node1, 4), (stage3, node1, 7)],
        0: [(stage5, node1, 0), (stage2, edge1, 1), (stage1, node0, 5), (stage3, edge1, 5), (stage4, edge1[:2], 8)],
    }

    def put_w2(layer, j, half, value, add):
        if add:
            G[layer, half, j, :, :H] += value[:H]
            G[layer, half, j, :, H:] += value[H:]
        else:
            G[layer, half, j, :, :H] = value[:H]
            G[layer, half, j, :, H:] = value[H:]

    def put_w1(layer, j, value, add=False):
        for half in range(2):
            if add:
                G[layer, half, j] += value[half * H:(half + 1) * H]
            else:
                G[layer, half, j] = value[half * H:(half + 1) * H]

    def mlp_bwd(d_msg, cen, hidden, gam, w2, layer, sm, j2, add):
        normed, inv_std = norm_parts(cen)
        sums = [sum_rows(d_msg * normed), sum_rows(d_msg)]
        d_normed = d_msg * gam
        d_out = inv_std * (d_normed - mean_cols(d_normed) - normed * mean_cols(d_normed * normed))
        sums = [sum_rows(d_out)] + sums
        d_out_bf = d_out.astype(BF)
        sig = gate(hidden)
        act = (hidden * sig).astype(BF)
        for half in range(2):
            put_w2(layer, j2, half, dot_rows(act, d_out_bf[:, half * H:(half + 1) * H]), add)
        d_hidden = second_t(d_out_bf, w2, layer) * (sig * (1.0 + hidden * (1.0 - sig)))
        sums = [sum_rows(d_hidden)] + sums
        for k in range(4):
            if add:
                SM[0, sm + k:sm + k + 1] += sums[k]
            else:
                SM[0, sm + k:sm + k + 1] = sums[k]
        return d_hidden.astype(BF)

    SM[...] = jnp.zeros_like(SM)

    def layer_bwd(layer, src):
        d_node = DN[...].astype(F32)
        d_hid = mlp_bwd(d_node, CN[layer], HN[layer], vec_row(layer, 1, True), W2N, layer, layer * 8, J_NW2, False)
        nodes, edge_w2, edge_w1 = (node1, edge1[:1], edge1[1:]) if layer else (node0, edge0[:1], edge0[1:])
        pl.semaphore_wait(csem.at[1 - layer], 3 if layer == 1 else 1)
        stage0(nodes[0])
        put_w1(layer, J_NW1, dot_rows(VF[layer], d_hid))
        stage0(nodes[1])
        put_w1(layer, J_NW1 + 1, dot_rows(SF[layer], d_hid))
        stage0(nodes[2])
        DV[...] = d_node + dot_cols(d_hid, full1(W1N, layer, 0))
        PS[...] = dot_cols(d_hid, full1(W1N, layer, 1)).reshape(NN, NS, D)
        for j in (J_EW2, J_EW1):
            G[layer, :, j] = jnp.zeros((2, H, D), F32)
        AG[...] = jnp.zeros_like(AG)
        PR[...] = jnp.zeros_like(PR)
        gam = vec_row(layer, 1, False)
        if layer == 0:
            for cp in fills:
                cp.wait()

        def edge(b, carry):
            for i in range(BE):
                GA[i * NS:(i + 1) * NS] = PS[rcv[b * BE + i]]
            d_edge = cat(rows_of(DE[0, edges(b)]), rows_of(DE[1, edges(b)]))
            d_hid = mlp_bwd(d_edge + GA[:BE * NS], CS[erows(b)], HS[erows(b)], gam, W2E, layer, layer * 8 + 4, J_EW2, True)
            lat = cat(rows_of(src[0, edges(b)]), rows_of(src[1, edges(b)])).astype(BF)
            put_w1(layer, J_EW1, dot_rows(lat, d_hid), True)
            new = d_edge + dot_cols(d_hid, full1(W1E, layer, 0))
            DE[0, edges(b)] = new[:, :H].reshape(BE, NS, H).astype(BF)
            DE[1, edges(b)] = new[:, H:].reshape(BE, NS, H).astype(BF)
            AG[...] += dot_rows(KS[erows(b)], d_hid)
            PR[...] += dot_rows(KR[erows(b)], d_hid).reshape(NN, NS, D)
            for stage, chunks, first in plan[layer]:
                for i, c in enumerate(chunks):
                    pl.when(b == first + i)(functools.partial(stage, c))
            return carry

        lax.fori_loop(0, NB, edge, 0)
        if layer == 1:
            for cp in fills:
                cp.start()
        run(stage0, edge_w2 + edge_w1[:1])
        d_ps, d_pr = AG[...].astype(BF), rows_of(PR[...]).astype(BF)
        put_w1(layer, J_EW1 + 1, dot_rows(VF[layer], d_ps))
        stage0(edge_w1[1])
        put_w1(layer, J_EW1 + 2, dot_rows(VF[layer], d_pr))
        stage0(edge_w1[2])
        DN[...] = (DV[...] + dot_cols(d_ps, full1(W1E, layer, 1))
                   + dot_cols(d_pr, full1(W1E, layer, 2))).astype(BF)

    layer_bwd(1, E1)
    run(stage1, edge1)
    run(stage4, node1)
    pl.semaphore_signal(csem.at[1], inc=1, device_id=partner, device_id_type=MESH)
    layer_bwd(0, E0)
    run(stage4, edge1[2:])
    run(stage1, edge0)

    pl.semaphore_signal(csem.at[2], inc=1, device_id=partner, device_id_type=MESH)
    run(stage2, node0)
    for k, ref in ((0, VF.at[2]), (1, DN)):
        rows = ref[...].astype(F32)
        NST[2 * k] = jnp.where(tp == 0, rows[:, :H], rows[:, H:]).reshape(NN, NS, H).astype(BF)
        NF[2 * k] = jnp.where(tp == 0, rows[:, H:], rows[:, :H]).reshape(NN, NS, H)

    def out_stage(b, carry):
        HS[erows(b), :H] = rows_of(E2[ot, edges(b)])
        HS[erows(b), H:] = rows_of(DE[ot, edges(b)])
        return carry

    lax.fori_loop(0, NB, out_stage, 0)
    pl.semaphore_wait(csem.at[2], 1)
    small0 = rdma(SM.at[0], SM.at[1], 2)
    small0.start()
    node_o = [rdma(NF.at[0], NF.at[1], 4), rdma(NF.at[2], NF.at[3], 5)]
    for cp in node_o:
        cp.start()

    out_copy = rdma(HS, CS, 6)
    out_copy.start()
    stores = [
        (E2.at[tp], o_e.at[:, mine]), (DE.at[tp], o_de.at[:, mine]),
        (NST.at[0], o_n.at[:, mine]), (NST.at[2], o_dn.at[:, mine]),
    ]
    run(stage5, edge1)
    stores = [pltpu.make_async_copy(src, dst, lsem.at[i]) for i, (src, dst) in enumerate(stores)]
    for cp in stores:
        cp.start()
    for k, cp in enumerate(node_o):
        cp.wait()
        NST[2 * k + 1] = NF[2 * k + 1].astype(BF)

    def out_recv(b, carry):
        E1[0, edges(b)] = CS[erows(b), :H].reshape(BE, NS, H).astype(BF)
        E1[1, edges(b)] = CS[erows(b), H:].reshape(BE, NS, H).astype(BF)
        return carry

    run(stage3, node0)
    out_copy.wait()
    lax.fori_loop(0, NB, out_recv, 0)
    more = [
        (E1.at[0], o_e.at[:, theirs]), (E1.at[1], o_de.at[:, theirs]),
        (NST.at[1], o_n.at[:, theirs]), (NST.at[3], o_dn.at[:, theirs]),
    ]
    more = [pltpu.make_async_copy(src, dst, lsem.at[6 + i]) for i, (src, dst) in enumerate(more)]
    for cp in more:
        cp.start()
    small0.wait()
    SM[2] = SM[0] + SM[1]
    small1 = rdma(SM.at[2], SM.at[3], 3, x_peer)
    small1.start()
    run(stage2, edge0)
    run(stage4, node0)
    small1.wait()
    SM[4] = SM[2] + SM[3]
    small2 = rdma(SM.at[4], SM.at[5], 13, y_peer)
    small2.start()
    run(stage3, edge0)
    small2.wait()
    total = SM[4] + SM[5]
    for layer in range(2):
        for row, ref_b, ref_v in ((0, o_bn, o_vn), (4, o_be, o_ve)):
            at = layer * 8 + row
            ref_b[layer:layer + 1] = total[at:at + 1]
            for k in range(3):
                one = total[at + 1 + k:at + 2 + k]
                ref_v[k, layer:layer + 1] = jnp.where(tp == 0, one[:, :H], one[:, H:])
    run(stage4, edge0)
    run(stage5, node0 + edge0)
    for c in node0 + edge0:
        wait_all(store_copies(c))
    for cp in stores + more:
        cp.wait()


def compute(*args):
    any_spec = pl.BlockSpec(memory_space=pl.ANY)
    vm = pl.BlockSpec(memory_space=pltpu.VMEM)
    sm = pl.BlockSpec(memory_space=pltpu.SMEM)
    v = pltpu.VMEM
    lat = (NN, 2 * NS, H)
    edg = (NE, 2 * NS, H)
    outs = [(lat, BF), (edg, BF), (lat, BF), (edg, BF),
            ((2, 3, H, D), F32), ((2, D, H), F32), ((2, 2, H, D), F32), ((2, D, H), F32),
            ((2, D), F32), ((2, D), F32), ((3, 2, H), F32), ((3, 2, H), F32), ((2, NE * NS, D), F32)]
    dma = pltpu.SemaphoreType.DMA
    node = (ROWS, D)
    scratch = [
        v((2, 3, 2, H, D), BF), v((2, 2, D, H), BF), v((2, 2, 2, H, D), BF), v((2, 2, D, H), BF),
        *[v((2, 3, 2, H), F32)] * 2, *[v((NE * NS, ROWS), BF)] * 2, *[v((2, NE, NS, H), BF)] * 4,
        v((NE * NS, D), F32), v((NE * NS, D), F32), v((7 * (H + 192), D), F32), v((2, 2, 7, H, D), F32),
        v((NN, NS, D), F32), v((NN, NS, D), F32), v((WIDE * NS, D), F32), v(node, F32),
        v((4, NN, NS, H), BF), v((4, NN, NS, H), F32),
        v((3, *node), BF), v((2, *node), BF), v((2, *node), F32), v((2, *node), F32),
        v(node, BF), v(node, F32), v((6, 16, D), F32),
        dma((12,)), dma((14,)), dma((14,)), pltpu.SemaphoreType.REGULAR((3,)), dma((4,)),
        dma((7, 3)), dma((7, 9)), dma((7, 2)),
    ]
    return pl.pallas_call(
        body,
        out_shape=[jax.ShapeDtypeStruct(*o) for o in outs],
        in_specs=[any_spec] * 8 + [vm] * 4 + [sm] * 2,
        out_specs=[any_spec] * 8 + [vm] * 4 + [any_spec],
        scratch_shapes=scratch,
        compiler_params=pltpu.CompilerParams(
            collective_id=0, has_side_effects=True, vmem_limit_bytes=67043328),
    )(*args)


def mover(*refs):
    n = (len(refs) - 2) // 3
    pieces = []
    for src, dst, buf in zip(refs[:n], refs[n:2 * n], refs[2 * n:]):
        step = -(-src.shape[0] // (4 if src.size > 1 << 18 else 1))
        for lo in range(0, src.shape[0], step):
            at = pl.ds(lo, min(step, src.shape[0] - lo))
            k = len(pieces)
            pieces.append((pltpu.make_async_copy(src.at[at], buf.at[at], refs[-2].at[k]),
                           pltpu.make_async_copy(buf.at[at], dst.at[at], refs[-1].at[k])))
    for get, unused in pieces:
        get.start()
    for get, put in pieces:
        get.wait()
        put.start()
    for unused, put in pieces:
        put.wait()


def move(arrays):
    any_spec = pl.BlockSpec(memory_space=pl.ANY)
    shapes = [jax.ShapeDtypeStruct(x.shape, x.dtype) for x in arrays]
    return pl.pallas_call(
        mover, out_shape=shapes, in_specs=[any_spec] * len(arrays), out_specs=[any_spec] * len(arrays),
        scratch_shapes=[pltpu.VMEM(x.shape, x.dtype) for x in arrays] + [pltpu.SemaphoreType.DMA((24,))] * 2,
        compiler_params=pltpu.CompilerParams(vmem_limit_bytes=67043328))(*arrays)


def solution(mesh):
    lat_spec = P('dp', None, 'tp')
    first_spec = P(None, None, 'tp', None)
    col_spec = P(None, None, 'tp')
    param_specs = (first_spec, P(), col_spec, col_spec, first_spec, P(), col_spec, col_spec)
    in_specs = (lat_spec, lat_spec, P(), P(), lat_spec, lat_spec) + param_specs
    out_specs = (lat_spec, lat_spec, lat_spec, lat_spec) + param_specs

    def local_step(node_lat, edge_lat, senders, receivers, grad_node, grad_edge, edge_w1, edge_b1, edge_w2, edge_vec, node_w1, node_b1, node_w2, node_vec):
        def swap(x):
            return jnp.transpose(x, (1, 0, 2))

        outs = compute(
            swap(node_lat), swap(edge_lat), swap(grad_node), swap(grad_edge), edge_w1, edge_w2, node_w1, node_w2,
            edge_b1, node_b1, swap(edge_vec), swap(node_vec), senders, receivers)
        outs = move(outs[:12])
        o_ew1, o_ew2, o_nw1, o_nw2, o_be, o_bn, o_ve, o_vn = outs[4:]
        return tuple(swap(x) for x in outs[:4]) + (o_ew1, o_be, o_ew2, swap(o_ve), o_nw1, o_bn, o_nw2, swap(o_vn))

    return jax.shard_map(local_step, mesh=mesh, in_specs=in_specs, out_specs=out_specs, check_vma=False)
```

```python
import functools

import jax
import jax.numpy as jnp
from jax import lax
from jax.experimental import pallas as pl
from jax.experimental.pallas import tpu as pltpu
from jax.sharding import PartitionSpec as P

BF = jnp.bfloat16
F32 = jnp.float32
MESH = pl.DeviceIdType.MESH
LN_EPS = 1e-5
NS = 8
NN = 42
NE = 300
D = 512
PAIR = 2 * NS
H = 256
ROWS = NN * NS
NB = 10
BE = NE // NB
WIDE = 60


def dot(lhs, rhs, lc=1, rc=0):
    return lax.dot_general(lhs, rhs, (((lc,), (rc,)), ((), ())), preferred_element_type=F32)


def dot_rows(lhs, rhs):
    return dot(lhs, rhs, 0)


def dot_cols(lhs, rhs):
    return dot(lhs, rhs, rc=1)


def cat(lhs, rhs):
    return jnp.concatenate([lhs, rhs], axis=1)


def mean_cols(x):
    return jnp.sum(x, axis=1, keepdims=True) * (1.0 / D)


def sum_rows(x):
    return jnp.sum(x, axis=0, keepdims=True)


def norm_parts(centered):
    inv_std = lax.rsqrt(mean_cols(centered * centered) + LN_EPS)
    return centered * inv_std, inv_std


J_NW2, J_NW1, J_EW2, J_EW1 = 0, 1, 3, 4


def rows_of(block):
    return block.astype(F32).reshape(block.shape[0] * NS, block.shape[2])


def body(nl, el, gn, ge, w1e, w2e, w1n, w2n, b1e, b1n, vece, vecn, snd, rcv,
         o_n, o_e, o_dn, o_de, o_ew1, o_ew2, o_nw1, o_nw2, o_be, o_bn, o_ve, o_vn, spill,
         W1E, W2E, W1N, W2N, VE, VN, KS, KR,
         E0, E1, E2, DE, HS, CS, R2, G, PS, PR, GA, AG,
         NST, NF, VF, SF, HN, CN, DN, DV, SM,
         lsem, ssem, rsem, csem, spsem, gssem, grsem, osem):
    dp = lax.axis_index('dp')
    tp = lax.axis_index('tp')
    ot = 1 - tp
    partner = (dp, ot)
    cx, cy = lax.rem(dp, 2), dp // 2
    x_peer = (cy * 2 + 1 - cx, tp)
    y_peer = ((1 - cy) * 2 + cx, tp)
    peers = (partner, x_peer, y_peer)

    def rdma(src, dst, idx, peer=None):
        return pltpu.make_async_remote_copy(
            src_ref=src, dst_ref=dst, send_sem=ssem.at[idx], recv_sem=rsem.at[idx],
            device_id=peer or partner, device_id_type=MESH)

    def wait_all(copies):
        for cp in copies:
            cp.wait()

    def start_all(copies):
        for cp in copies:
            cp.start()

    mine = pl.ds(pl.multiple_of(tp * NS, NS), NS)
    theirs = pl.ds(pl.multiple_of(ot * NS, NS), NS)
    loads = [
        (nl.at[:, mine], NST.at[0]), (nl.at[:, theirs], NST.at[1]),
        (w1e, W1E.at[:, :, tp]), (el.at[:, theirs], E1.at[0]), (w2e, W2E.at[:, tp]),
        (el.at[:, mine], E0.at[tp]), (w1n, W1N.at[:, :, tp]), (w2n, W2N.at[:, tp]),
        (ge.at[:, theirs], E1.at[1]), (ge.at[:, mine], DE.at[tp]),
        (gn.at[:, mine], NST.at[2]), (gn.at[:, theirs], NST.at[3]),
    ]
    loads = [pltpu.make_async_copy(src, dst, lsem.at[i]) for i, (src, dst) in enumerate(loads)]
    for cp in loads:
        cp.start()

    barrier = pltpu.get_barrier_semaphore()
    for peer in peers:
        pl.semaphore_signal(barrier, inc=1, device_id=peer, device_id_type=MESH)
    loads[0].wait()
    loads[1].wait()
    NF[0] = NST[1].astype(F32)
    pl.semaphore_wait(barrier, 3)
    vec_copies = [rdma(vece, VE.at[tp], 0), rdma(vecn, VN.at[tp], 1)]
    for cp in vec_copies:
        cp.start()
    VE[tp] = vece[...]
    VN[tp] = vecn[...]

    node_x = rdma(NF.at[0], NF.at[1], 2)
    node_x.start()

    def w_pack(layer, j):
        if j == J_NW2:
            half = W2N[layer, tp]
        elif j == J_EW2:
            half = W2E[layer, tp]
        elif j < J_EW2:
            return W1N[layer, j - J_NW1, tp].astype(F32)
        else:
            return W1E[layer, j - J_EW1, tp].astype(F32)
        half = half.astype(F32)
        return cat(half[:H], half[H:])

    def w_unpack(layer, j, block):
        block = block.astype(BF)
        if j in (J_NW2, J_EW2):
            ref = W2N if j == J_NW2 else W2E
            ref[layer, ot, :H] = block[:, :H]
            ref[layer, ot, H:] = block[:, H:]
        elif j < J_EW2:
            W1N[layer, j - J_NW1, ot] = block
        else:
            W1E[layer, j - J_EW1, ot] = block

    groups = [(0, J_EW1 + 1, 2), (0, J_EW1, 1), (0, J_EW2, 1), (0, 0, 3), (1, 0, 7)]
    w_copies = [rdma(G.at[1, layer, pl.ds(lo, n)], G.at[0, layer, pl.ds(lo, n)], 8 + k)
                for k, (layer, lo, n) in enumerate(groups)]

    def w_packs(k):
        layer, lo, n = groups[k]
        for j in range(lo, lo + n):
            G[1, layer, j] = w_pack(layer, j)

    def w_recv(k):
        layer, lo, n = groups[k]
        w_copies[k].wait()
        for j in range(lo, lo + n):
            w_unpack(layer, j, G[0, layer, j])

    def edges(b, n=BE):
        return pl.ds(b * n, n)

    def erows(b, n=BE):
        return pl.ds(pl.multiple_of(b * n * NS, n * NS), n * NS)

    def lat_copy(b):
        at = erows(b, WIDE)
        return rdma(HS.at[at, :H], CS.at[at, :H], 14 + b)

    grad_copy = rdma(R2.at[:NE * NS, :H], R2.at[:NE * NS, H:], 7)

    def stage_rows(dst, src):
        def one(b, carry):
            dst[erows(b), :H] = rows_of(src[edges(b)])
            return carry
        lax.fori_loop(0, NB, one, 0)

    loads[2].wait()
    for k in range(2):
        w_packs(k)
        w_copies[k].start()
    wait_all(loads[3:5])
    stage_rows(HS, E1.at[0])
    lat_copy(0).start()
    w_packs(2)
    w_copies[2].start()
    lat_copy(1).start()
    wait_all(loads[5:])
    w_packs(3)
    w_packs(4)
    stage_rows(R2, E1.at[1])
    NF[2] = NST[3].astype(F32)
    node_g = rdma(NF.at[2], NF.at[3], 3)

    column = lax.broadcasted_iota(jnp.int32, (NS, ROWS), 1) - lax.broadcasted_iota(jnp.int32, (NS, ROWS), 0)

    def select(dst, ids):
        def one(i, carry):
            two = [jnp.where(column == ids[2 * i + k] * NS, 1.0, 0.0) for k in range(2)]
            at = pl.ds(pl.multiple_of(i * PAIR, PAIR), PAIR)
            dst[at] = jnp.concatenate(two, axis=0).astype(BF)
            return carry
        lax.fori_loop(0, NE // 2, one, 0, unroll=5)

    select(KR, rcv)

    def node_in(dst, staged, received):
        own, got = rows_of(NST[staged]), rows_of(NF[received])
        lo = jnp.where(tp == 0, own, got)
        hi = jnp.where(tp == 0, got, own)
        dst[...] = cat(lo, hi).astype(BF)

    for cp in vec_copies:
        cp.wait()
    node_x.wait()
    node_in(VF.at[0], 0, 1)

    def vec_row(layer, row, node=False):
        ref = VN if node else VE
        return cat(ref[0, row, layer:layer + 1], ref[1, row, layer:layer + 1])

    def full1(ref, layer, k):
        return ref[layer, k].reshape(D, D)

    def gate(hidden):
        return 0.5 + 0.5 * jnp.tanh(0.5 * hidden)

    def second(act, ref, layer):
        return cat(dot(act, ref[layer, 0]), dot(act, ref[layer, 1]))

    def second_t(dout, ref, layer):
        return dot_cols(dout[:, :H], ref[layer, 0]) + dot_cols(dout[:, H:], ref[layer, 1])

    def add_message(dst, b, n, lat, msg):
        new = lat + msg.astype(F32)
        dst[0, edges(b, n)] = new[:, :H].reshape(n, NS, H).astype(BF)
        dst[1, edges(b, n)] = new[:, H:].reshape(n, NS, H).astype(BF)

    def layer_fwd(layer, src, dst):
        w_recv(4 * layer)
        PS[...] = (dot(VF[layer], full1(W1E, layer, 1)) + b1e[layer:layer + 1]).reshape(NN, NS, D)
        PR[...] = dot(VF[layer], full1(W1E, layer, 2)).reshape(NN, NS, D)
        if layer:
            start_all([grad_copy, node_g])
        else:
            w_recv(1)
            w_recv(2)
            lat_copy(2).start()
        c0, gam, bet = (vec_row(layer, r) for r in range(3))
        AG[...] = jnp.zeros_like(AG)

        def edge(b, carry):
            if not layer:
                lat_copy(b).wait()
                pl.when(b < 2)(lambda: lat_copy(b + 3).start())
                pl.when(b == 2)(w_copies[3].start)
                pl.when(b == 3)(w_copies[4].start)
                src[ot, edges(b, WIDE)] = CS[erows(b, WIDE), :H].reshape(WIDE, NS, H).astype(BF)
            for i in range(WIDE):
                GA[i * NS:(i + 1) * NS] = PS[snd[b * WIDE + i]] + PR[rcv[b * WIDE + i]]
            lat = cat(rows_of(src[0, edges(b, WIDE)]), rows_of(src[1, edges(b, WIDE)]))
            hidden = dot(lat.astype(BF), full1(W1E, layer, 0)) + GA[...]
            HS[erows(b, WIDE)] = hidden
            act = (hidden * gate(hidden)).astype(BF)
            out = second(act, W2E, layer) + c0
            cen = out - mean_cols(out)
            CS[erows(b, WIDE)] = cen
            normed, unused = norm_parts(cen)
            msg = (normed * gam + bet).astype(BF)
            AG[...] += dot_rows(KR[erows(b, WIDE)], msg)
            if not layer:
                add_message(dst, b, WIDE, lat, msg)
            return carry

        lax.fori_loop(0, NE // WIDE, edge, 0)
        if not layer:
            start_all(spills)
            w_recv(3)
        SF[layer] = AG[...].astype(BF)
        lat = VF[layer]
        hidden = dot(lat, full1(W1N, layer, 0)) + dot(SF[layer], full1(W1N, layer, 1)) + b1n[layer:layer + 1]
        HN[layer] = hidden
        act = (hidden * gate(hidden)).astype(BF)
        out = second(act, W2N, layer) + vec_row(layer, 0, True)
        cen = out - mean_cols(out)
        CN[layer] = cen
        normed, unused = norm_parts(cen)
        msg = (normed * vec_row(layer, 1, True) + vec_row(layer, 2, True)).astype(BF)
        VF[layer + 1] = (lat.astype(F32) + msg.astype(F32)).astype(BF)

    spills = [pltpu.make_async_copy(HS, spill.at[0], spsem.at[0]), pltpu.make_async_copy(CS, spill.at[1], spsem.at[1])]
    fills = [pltpu.make_async_copy(spill.at[0], HS, spsem.at[2]), pltpu.make_async_copy(spill.at[1], CS, spsem.at[3])]

    layer_fwd(0, E0, E1)
    select(KS, snd)
    wait_all(spills)
    layer_fwd(1, E1, None)
    grad_copy.wait()

    def grad_rows(b, carry):
        DE[ot, edges(b)] = R2[erows(b), H:].reshape(BE, NS, H).astype(BF)
        return carry

    lax.fori_loop(0, NB, grad_rows, 0)
    for peer in peers:
        pl.semaphore_signal(csem.at[0], inc=1, device_id=peer, device_id_type=MESH)
    node_g.wait()
    node_in(DN, 2, 3)

    def chunk(c):
        return 1 - c // 7, c % 7

    def g_copy(c, send, k, src, dst, peer):
        return pltpu.make_async_remote_copy(
            src_ref=src, dst_ref=dst, send_sem=gssem.at[c % 7, send], recv_sem=grsem.at[c % 7, k],
            device_id=peer, device_id_type=MESH)

    def core_copy(c):
        layer, j = chunk(c)
        return g_copy(c, 0, 0, G.at[layer, ot, j], R2.at[j * H:(j + 1) * H], partner)

    def landing(c):
        layer, j = chunk(c)
        if layer:
            return lambda lo, n: R2.at[7 * H + j * 192 + lo:7 * H + j * 192 + lo + n]
        return lambda lo, n: G.at[1, tp, j, lo:lo + n]

    half_p, half_q = cx * 64, 128 + cy * 64
    quarter_p, quarter_q = half_p + cy * 32, half_q + cx * 32

    def strip(c, start, n, final=False):
        layer, j = chunk(c)
        return G.at[layer, ot if final else tp, j, pl.ds(pl.multiple_of(start, 32), n)]

    def a_copies(c):
        land = landing(c)
        return [g_copy(c, 1, 1, strip(c, 64 - half_p, 64), land(0, 64), x_peer),
                g_copy(c, 2, 2, strip(c, 320 - half_q, 64), land(64, 64), y_peer)]

    def b_copies(c):
        land = landing(c)
        return [g_copy(c, 1, 3, strip(c, half_p + 32 - cy * 32, 32), land(128, 32), y_peer),
                g_copy(c, 2, 4, strip(c, half_q + 32 - cx * 32, 32), land(160, 32), x_peer)]

    def c_copies(c):
        ref_p, ref_q = strip(c, quarter_p, 32, True), strip(c, quarter_q, 32, True)
        return [g_copy(c, 1, 5, ref_p, ref_p, y_peer), g_copy(c, 2, 6, ref_q, ref_q, x_peer)]

    def d_copies(c):
        ref_p, ref_q = strip(c, half_p, 64, True), strip(c, half_q, 64, True)
        return [g_copy(c, 1, 7, ref_p, ref_p, x_peer), g_copy(c, 2, 8, ref_q, ref_q, y_peer)]

    def store_copies(c):
        layer, j = chunk(c)
        src = G.at[layer, ot, j]
        if j in (J_NW2, J_EW2):
            ref = o_nw2 if j == J_NW2 else o_ew2
            pairs = [(src.at[:, :H], ref.at[layer, :H]), (src.at[:, H:], ref.at[layer, H:])]
        elif j < J_EW2:
            pairs = [(src, o_nw1.at[layer, j - J_NW1])]
        else:
            pairs = [(src, o_ew1.at[layer, j - J_EW1])]
        return [pltpu.make_async_copy(a, b, osem.at[c % 7, k]) for k, (a, b) in enumerate(pairs)]

    def stage0(c):
        core_copy(c).start()

    def stage1(c):
        layer, j = chunk(c)
        core_copy(c).wait()
        G[layer, tp, j] += R2[j * H:(j + 1) * H]
        start_all(a_copies(c))

    def stage2(c):
        land = landing(c)
        wait_all(a_copies(c))
        for start, lo in ((half_p, 0), (half_q, 64)):
            ref = strip(c, start, 64)
            ref[...] += land(lo, 64)[...]
        start_all(b_copies(c))

    def stage3(c):
        land = landing(c)
        wait_all(b_copies(c))
        for start, lo in ((quarter_p, 128), (quarter_q, 160)):
            strip(c, start, 32, True)[...] = strip(c, start, 32)[...] + land(lo, 32)[...]
        start_all(c_copies(c))

    def stage4(c):
        wait_all(c_copies(c))
        start_all(d_copies(c))

    def stage5(c):
        wait_all(d_copies(c))
        if c >= 7:
            wait_all(store_copies(c - 7))
        start_all(store_copies(c))

    def run(stage, chunks):
        for c in chunks:
            stage(c)

    node1, edge1, node0, edge0 = (list(range(*ends)) for ends in ((0, 3), (3, 7), (7, 10), (10, 14)))

    plan = {
        1: [(stage2, node1, 3), (stage3, node1, 7)],
        0: [(stage2, edge1, 0), (stage5, node1, 3), (stage3, edge1, 5), (stage4, edge1[:2], 8)],
    }

    def put_w2(layer, j, half, value, add):
        if add:
            G[layer, half, j, :, :H] += value[:H]
            G[layer, half, j, :, H:] += value[H:]
        else:
            G[layer, half, j, :, :H] = value[:H]
            G[layer, half, j, :, H:] = value[H:]

    def put_w1(layer, j, value, add=False):
        for half in range(2):
            if add:
                G[layer, half, j] += value[half * H:(half + 1) * H]
            else:
                G[layer, half, j] = value[half * H:(half + 1) * H]

    def mlp_bwd(d_msg, cen, hidden, gam, w2, layer, sm, j2, add):
        normed, inv_std = norm_parts(cen)
        sums = [sum_rows(d_msg * normed), sum_rows(d_msg)]
        d_normed = d_msg * gam
        d_out = inv_std * (d_normed - mean_cols(d_normed) - normed * mean_cols(d_normed * normed))
        sums = [sum_rows(d_out)] + sums
        d_out_bf = d_out.astype(BF)
        sig = gate(hidden)
        act = (hidden * sig).astype(BF)
        for half in range(2):
            put_w2(layer, j2, half, dot_rows(act, d_out_bf[:, half * H:(half + 1) * H]), add)
        d_hidden = second_t(d_out_bf, w2, layer) * (sig * (1.0 + hidden * (1.0 - sig)))
        sums = [sum_rows(d_hidden)] + sums
        for k in range(4):
            if add:
                SM[0, sm + k:sm + k + 1] += sums[k]
            else:
                SM[0, sm + k:sm + k + 1] = sums[k]
        return d_hidden.astype(BF)

    SM[...] = jnp.zeros_like(SM)

    def layer_bwd(layer, src):
        d_node = DN[...].astype(F32)
        d_hid = mlp_bwd(d_node, CN[layer], HN[layer], vec_row(layer, 1, True), W2N, layer, layer * 8, J_NW2, False)
        nodes, edge_w2, edge_w1 = (node1, edge1[:1], edge1[1:]) if layer else (node0, edge0[:1], edge0[1:])
        pl.semaphore_wait(csem.at[1 - layer], 3 if layer == 1 else 1)
        stage0(nodes[0])
        put_w1(layer, J_NW1, dot_rows(VF[layer], d_hid))
        stage0(nodes[1])
        stage1(nodes[0])
        put_w1(layer, J_NW1 + 1, dot_rows(SF[layer], d_hid))
        stage0(nodes[2])
        stage1(nodes[1])
        DV[...] = d_node + dot_cols(d_hid, full1(W1N, layer, 0))
        PS[...] = dot_cols(d_hid, full1(W1N, layer, 1)).reshape(NN, NS, D)
        stage1(nodes[2])
        for j in (J_EW2, J_EW1):
            G[layer, :, j] = jnp.zeros((2, H, D), F32)
        AG[...] = jnp.zeros_like(AG)
        PR[...] = jnp.zeros_like(PR)
        gam, bet = vec_row(layer, 1), vec_row(layer, 2)
        if not layer:
            for cp in fills:
                cp.wait()

        def edge(b, carry):
            for i in range(BE):
                GA[i * NS:(i + 1) * NS] = PS[rcv[b * BE + i]]
            d_edge = cat(rows_of(DE[0, edges(b)]), rows_of(DE[1, edges(b)]))
            d_hid = mlp_bwd(d_edge + GA[:BE * NS], CS[erows(b)], HS[erows(b)], gam, W2E, layer, layer * 8 + 4, J_EW2, True)
            lat = cat(rows_of(src[0, edges(b)]), rows_of(src[1, edges(b)]))
            put_w1(layer, J_EW1, dot_rows(lat.astype(BF), d_hid), True)
            if layer:
                normed, unused = norm_parts(CS[erows(b)])
                add_message(E2, b, BE, lat, (normed * gam + bet).astype(BF))
            new = d_edge + dot_cols(d_hid, full1(W1E, layer, 0))
            DE[0, edges(b)] = new[:, :H].reshape(BE, NS, H).astype(BF)
            DE[1, edges(b)] = new[:, H:].reshape(BE, NS, H).astype(BF)
            AG[...] += dot_rows(KS[erows(b)], d_hid)
            PR[...] += dot_rows(KR[erows(b)], d_hid).reshape(NN, NS, D)
            for stage, chunks, first in plan[layer]:
                for i, c in enumerate(chunks):
                    pl.when(b == first + i)(functools.partial(stage, c))
            return carry

        lax.fori_loop(0, NB, edge, 0)
        if layer:
            for cp in fills:
                cp.start()
        run(stage0, edge_w2 + edge_w1[:1])
        run(stage4, node1[:2] if layer else edge1[2:])
        d_ps, d_pr = AG[...].astype(BF), rows_of(PR[...]).astype(BF)
        put_w1(layer, J_EW1 + 1, dot_rows(VF[layer], d_ps))
        stage0(edge_w1[1])
        put_w1(layer, J_EW1 + 2, dot_rows(VF[layer], d_pr))
        stage0(edge_w1[2])
        DN[...] = (DV[...] + dot_cols(d_ps, full1(W1E, layer, 1))
                   + dot_cols(d_pr, full1(W1E, layer, 2))).astype(BF)

    layer_bwd(1, E1)
    run(stage1, edge1)
    run(stage4, node1[2:])
    pl.semaphore_signal(csem.at[1], inc=1, device_id=partner, device_id_type=MESH)
    layer_bwd(0, E0)
    run(stage1, edge0)

    pl.semaphore_signal(csem.at[2], inc=1, device_id=partner, device_id_type=MESH)
    run(stage2, node0)
    for k, ref in ((0, VF.at[2]), (1, DN)):
        rows = ref[...].astype(F32)
        NST[2 * k] = jnp.where(tp == 0, rows[:, :H], rows[:, H:]).reshape(NN, NS, H).astype(BF)
        NF[2 * k] = jnp.where(tp == 0, rows[:, H:], rows[:, :H]).reshape(NN, NS, H)

    def out_stage(b, carry):
        HS[erows(b), :H] = rows_of(E2[ot, edges(b)])
        HS[erows(b), H:] = rows_of(DE[ot, edges(b)])
        return carry

    lax.fori_loop(0, NB, out_stage, 0)
    pl.semaphore_wait(csem.at[2], 1)
    small0 = rdma(SM.at[0], SM.at[1], 2)
    small0.start()
    node_o = [rdma(NF.at[0], NF.at[1], 4), rdma(NF.at[2], NF.at[3], 5)]
    for cp in node_o:
        cp.start()

    out_copy = rdma(HS, CS, 6)
    out_copy.start()
    stores = [
        (E2.at[tp], o_e.at[:, mine]), (DE.at[tp], o_de.at[:, mine]),
        (NST.at[0], o_n.at[:, mine]), (NST.at[2], o_dn.at[:, mine]),
    ]
    run(stage5, edge1)
    stores = [pltpu.make_async_copy(src, dst, lsem.at[i]) for i, (src, dst) in enumerate(stores)]
    for cp in stores:
        cp.start()
    for k, cp in enumerate(node_o):
        cp.wait()
        NST[2 * k + 1] = NF[2 * k + 1].astype(BF)

    def out_recv(b, carry):
        E1[0, edges(b)] = CS[erows(b), :H].reshape(BE, NS, H).astype(BF)
        E1[1, edges(b)] = CS[erows(b), H:].reshape(BE, NS, H).astype(BF)
        return carry

    run(stage3, node0)
    out_copy.wait()
    lax.fori_loop(0, NB, out_recv, 0)
    more = [
        (E1.at[0], o_e.at[:, theirs]), (E1.at[1], o_de.at[:, theirs]),
        (NST.at[1], o_n.at[:, theirs]), (NST.at[3], o_dn.at[:, theirs]),
    ]
    more = [pltpu.make_async_copy(src, dst, lsem.at[6 + i]) for i, (src, dst) in enumerate(more)]
    for cp in more:
        cp.start()
    small0.wait()
    SM[2] = SM[0] + SM[1]
    small1 = rdma(SM.at[2], SM.at[3], 3, x_peer)
    small1.start()
    run(stage2, edge0)
    run(stage4, node0)
    small1.wait()
    SM[4] = SM[2] + SM[3]
    small2 = rdma(SM.at[4], SM.at[5], 13, y_peer)
    small2.start()
    run(stage3, edge0)
    small2.wait()
    total = SM[4] + SM[5]
    for layer in range(2):
        for row, ref_b, ref_v in ((0, o_bn, o_vn), (4, o_be, o_ve)):
            at = layer * 8 + row
            ref_b[layer:layer + 1] = total[at:at + 1]
            for k in range(3):
                one = total[at + 1 + k:at + 2 + k]
                ref_v[k, layer:layer + 1] = jnp.where(tp == 0, one[:, :H], one[:, H:])
    run(stage4, edge0)
    run(stage5, node0 + edge0)
    for c in node0 + edge0:
        wait_all(store_copies(c))
    for cp in stores + more:
        cp.wait()


def compute(*args):
    any_spec = pl.BlockSpec(memory_space=pl.ANY)
    vm = pl.BlockSpec(memory_space=pltpu.VMEM)
    sm = pl.BlockSpec(memory_space=pltpu.SMEM)
    v = pltpu.VMEM
    lat = (NN, 2 * NS, H)
    edg = (NE, 2 * NS, H)
    outs = [(lat, BF), (edg, BF), (lat, BF), (edg, BF),
            ((2, 3, H, D), F32), ((2, D, H), F32), ((2, 2, H, D), F32), ((2, D, H), F32),
            ((2, D), F32), ((2, D), F32), ((3, 2, H), F32), ((3, 2, H), F32), ((2, NE * NS, D), F32)]
    dma = pltpu.SemaphoreType.DMA
    node = (ROWS, D)
    scratch = [
        v((2, 3, 2, H, D), BF), v((2, 2, D, H), BF), v((2, 2, 2, H, D), BF), v((2, 2, D, H), BF),
        *[v((2, 3, 2, H), F32)] * 2, *[v((NE * NS, ROWS), BF)] * 2, *[v((2, NE, NS, H), BF)] * 4,
        v((NE * NS, D), F32), v((NE * NS, D), F32), v((7 * (H + 192), D), F32), v((2, 2, 7, H, D), F32),
        v((NN, NS, D), F32), v((NN, NS, D), F32), v((WIDE * NS, D), F32), v(node, F32),
        v((4, NN, NS, H), BF), v((4, NN, NS, H), F32),
        v((3, *node), BF), v((2, *node), BF), v((2, *node), F32), v((2, *node), F32),
        v(node, BF), v(node, F32), v((6, 16, D), F32),
        dma((12,)), dma((19,)), dma((19,)), pltpu.SemaphoreType.REGULAR((3,)), dma((4,)),
        dma((7, 3)), dma((7, 9)), dma((7, 2)),
    ]
    return pl.pallas_call(
        body,
        out_shape=[jax.ShapeDtypeStruct(*o) for o in outs],
        in_specs=[any_spec] * 8 + [vm] * 4 + [sm] * 2,
        out_specs=[any_spec] * 8 + [vm] * 4 + [any_spec],
        scratch_shapes=scratch,
        compiler_params=pltpu.CompilerParams(
            collective_id=0, has_side_effects=True, vmem_limit_bytes=67043328),
    )(*args)


def mover(*refs):
    n = (len(refs) - 2) // 3
    pieces = []
    for src, dst, buf in zip(refs[:n], refs[n:2 * n], refs[2 * n:]):
        step = -(-src.shape[0] // (4 if src.size > 1 << 18 else 1))
        for lo in range(0, src.shape[0], step):
            at = pl.ds(lo, min(step, src.shape[0] - lo))
            k = len(pieces)
            pieces.append((pltpu.make_async_copy(src.at[at], buf.at[at], refs[-2].at[k]),
                           pltpu.make_async_copy(buf.at[at], dst.at[at], refs[-1].at[k])))
    for get, unused in pieces:
        get.start()
    for get, put in pieces:
        get.wait()
        put.start()
    for unused, put in pieces:
        put.wait()


def move(arrays):
    any_spec = pl.BlockSpec(memory_space=pl.ANY)
    shapes = [jax.ShapeDtypeStruct(x.shape, x.dtype) for x in arrays]
    return pl.pallas_call(
        mover, out_shape=shapes, in_specs=[any_spec] * len(arrays), out_specs=[any_spec] * len(arrays),
        scratch_shapes=[pltpu.VMEM(x.shape, x.dtype) for x in arrays] + [pltpu.SemaphoreType.DMA((24,))] * 2,
        compiler_params=pltpu.CompilerParams(vmem_limit_bytes=67043328))(*arrays)


def solution(mesh):
    lat_spec = P('dp', None, 'tp')
    first_spec = P(None, None, 'tp', None)
    col_spec = P(None, None, 'tp')
    param_specs = (first_spec, P(), col_spec, col_spec, first_spec, P(), col_spec, col_spec)
    in_specs = (lat_spec, lat_spec, P(), P(), lat_spec, lat_spec) + param_specs
    out_specs = (lat_spec, lat_spec, lat_spec, lat_spec) + param_specs

    def local_step(node_lat, edge_lat, senders, receivers, grad_node, grad_edge, edge_w1, edge_b1, edge_w2, edge_vec, node_w1, node_b1, node_w2, node_vec):
        def swap(x):
            return jnp.transpose(x, (1, 0, 2))

        outs = compute(
            swap(node_lat), swap(edge_lat), swap(grad_node), swap(grad_edge), edge_w1, edge_w2, node_w1, node_w2,
            edge_b1, node_b1, swap(edge_vec), swap(node_vec), senders, receivers)
        outs = move(outs[:12])
        o_ew1, o_ew2, o_nw1, o_nw2, o_be, o_bn, o_ve, o_vn = outs[4:]
        return tuple(swap(x) for x in outs[:4]) + (o_ew1, o_be, o_ew2, swap(o_ve), o_nw1, o_bn, o_nw2, swap(o_vn))

    return jax.shard_map(local_step, mesh=mesh, in_specs=in_specs, out_specs=out_specs, check_vma=False)
```

```python
import functools

import jax
import jax.numpy as jnp
from jax import lax
from jax.experimental import pallas as pl
from jax.experimental.pallas import tpu as pltpu
from jax.sharding import PartitionSpec as P

BF = jnp.bfloat16
F32 = jnp.float32
MESH = pl.DeviceIdType.MESH
LN_EPS = 1e-5
NS = 8
NN = 42
NE = 300
D = 512
PAIR = 2 * NS
H = 256
ROWS = NN * NS
NB = 5
BE = NE // NB
WIDE = 60


def dot(lhs, rhs, lc=1, rc=0):
    return lax.dot_general(lhs, rhs, (((lc,), (rc,)), ((), ())), preferred_element_type=F32)


def dot_rows(lhs, rhs):
    return dot(lhs, rhs, 0)


def dot_cols(lhs, rhs):
    return dot(lhs, rhs, rc=1)


def cat(lhs, rhs):
    return jnp.concatenate([lhs, rhs], axis=1)


def mean_cols(x):
    return jnp.sum(x, axis=1, keepdims=True) * (1.0 / D)


def sum_rows(x):
    return jnp.sum(x, axis=0, keepdims=True)


def norm_parts(centered):
    inv_std = lax.rsqrt(mean_cols(centered * centered) + LN_EPS)
    return centered * inv_std, inv_std


J_NW2, J_NW1, J_EW2, J_EW1 = 0, 1, 3, 4


def rows_of(block):
    return block.astype(F32).reshape(block.shape[0] * NS, block.shape[2])


def body(nl, el, gn, ge, w1e, w2e, w1n, w2n, b1e, b1n, vece, vecn, snd, rcv,
         o_n, o_e, o_dn, o_de, o_ew1, o_ew2, o_nw1, o_nw2, o_be, o_bn, o_ve, o_vn, spill,
         W1E, W2E, W1N, W2N, VE, VN, KS, KR,
         E0, E1, E2, DE, HS, CS, R2, G, PS, PR, GA, AG,
         NST, NF, VF, SF, HN, CN, DN, SM,
         lsem, ssem, rsem, csem, spsem, gssem, grsem, osem):
    dp = lax.axis_index('dp')
    tp = lax.axis_index('tp')
    ot = 1 - tp
    partner = (dp, ot)
    cx, cy = lax.rem(dp, 2), dp // 2
    x_peer = (cy * 2 + 1 - cx, tp)
    y_peer = ((1 - cy) * 2 + cx, tp)
    peers = (partner, x_peer, y_peer)

    def rdma(src, dst, idx, peer=None):
        return pltpu.make_async_remote_copy(
            src_ref=src, dst_ref=dst, send_sem=ssem.at[idx], recv_sem=rsem.at[idx],
            device_id=peer or partner, device_id_type=MESH)

    def wait_all(copies):
        for cp in copies:
            cp.wait()

    def start_all(copies):
        for cp in copies:
            cp.start()

    mine = pl.ds(pl.multiple_of(tp * NS, NS), NS)
    theirs = pl.ds(pl.multiple_of(ot * NS, NS), NS)
    loads = [
        (nl.at[:, mine], NST.at[0]), (nl.at[:, theirs], NST.at[1]),
        (w1e, W1E.at[:, :, tp]), (el.at[:, theirs], E1.at[0]), (w2e, W2E.at[:, tp]),
        (el.at[:, mine], E0.at[tp]), (w1n, W1N.at[:, :, tp]), (w2n, W2N.at[:, tp]),
        (ge.at[:, theirs], E1.at[1]), (ge.at[:, mine], DE.at[tp]),
        (gn.at[:, mine], NST.at[2]), (gn.at[:, theirs], NST.at[3]),
    ]
    loads = [pltpu.make_async_copy(src, dst, lsem.at[i]) for i, (src, dst) in enumerate(loads)]
    for cp in loads:
        cp.start()

    barrier = pltpu.get_barrier_semaphore()
    for peer in peers:
        pl.semaphore_signal(barrier, inc=1, device_id=peer, device_id_type=MESH)
    loads[0].wait()
    loads[1].wait()
    NF[0] = NST[1].astype(F32)
    pl.semaphore_wait(barrier, 3)
    vec_copies = [rdma(vece, VE.at[tp], 0), rdma(vecn, VN.at[tp], 1)]
    for cp in vec_copies:
        cp.start()
    VE[tp] = vece[...]
    VN[tp] = vecn[...]

    node_x = rdma(NF.at[0], NF.at[1], 2)
    node_x.start()

    def w_pack(layer, j):
        if j == J_NW2:
            half = W2N[layer, tp]
        elif j == J_EW2:
            half = W2E[layer, tp]
        elif j < J_EW2:
            return W1N[layer, j - J_NW1, tp].astype(F32)
        else:
            return W1E[layer, j - J_EW1, tp].astype(F32)
        half = half.astype(F32)
        return cat(half[:H], half[H:])

    def w_unpack(layer, j, block):
        block = block.astype(BF)
        if j in (J_NW2, J_EW2):
            ref = W2N if j == J_NW2 else W2E
            ref[layer, ot, :H] = block[:, :H]
            ref[layer, ot, H:] = block[:, H:]
        elif j < J_EW2:
            W1N[layer, j - J_NW1, ot] = block
        else:
            W1E[layer, j - J_EW1, ot] = block

    groups = [(0, J_EW1 + 1, 2), (0, J_EW1, 1), (0, J_EW2, 1), (0, 0, 3), (1, 0, 7)]
    w_copies = [rdma(G.at[1, layer, pl.ds(lo, n)], G.at[0, layer, pl.ds(lo, n)], 8 + k)
                for k, (layer, lo, n) in enumerate(groups)]

    def w_packs(k):
        layer, lo, n = groups[k]
        for j in range(lo, lo + n):
            G[1, layer, j] = w_pack(layer, j)

    def w_recv(k):
        layer, lo, n = groups[k]
        w_copies[k].wait()
        for j in range(lo, lo + n):
            w_unpack(layer, j, G[0, layer, j])

    def edges(b, n=BE):
        return pl.ds(b * n, n)

    def erows(b, n=BE):
        return pl.ds(pl.multiple_of(b * n * NS, n * NS), n * NS)

    def lat_copy(b):
        at = erows(b, WIDE)
        return rdma(HS.at[at, :H], CS.at[at, :H], 14 + b)

    grad_copy = rdma(R2.at[:NE * NS, :H], R2.at[:NE * NS, H:], 7)

    def stage_rows(dst, src):
        def one(b, carry):
            dst[erows(b), :H] = rows_of(src[edges(b)])
            return carry
        lax.fori_loop(0, NB, one, 0)

    loads[2].wait()
    for k in range(2):
        w_packs(k)
        w_copies[k].start()
    wait_all(loads[3:5])
    stage_rows(HS, E1.at[0])
    lat_copy(0).start()
    w_packs(2)
    w_copies[2].start()
    lat_copy(1).start()
    wait_all(loads[5:])
    w_packs(3)
    w_packs(4)
    stage_rows(R2, E1.at[1])
    NF[2] = NST[3].astype(F32)
    node_g = rdma(NF.at[2], NF.at[3], 3)

    column = lax.broadcasted_iota(jnp.int32, (NS, ROWS), 1) - lax.broadcasted_iota(jnp.int32, (NS, ROWS), 0)

    def select(dst, ids):
        def one(i, carry):
            two = [jnp.where(column == ids[2 * i + k] * NS, 1.0, 0.0) for k in range(2)]
            at = pl.ds(pl.multiple_of(i * PAIR, PAIR), PAIR)
            dst[at] = jnp.concatenate(two, axis=0).astype(BF)
            return carry
        lax.fori_loop(0, NE // 2, one, 0, unroll=5)

    select(KR, rcv)

    def node_in(dst, staged, received):
        own, got = rows_of(NST[staged]), rows_of(NF[received])
        lo = jnp.where(tp == 0, own, got)
        hi = jnp.where(tp == 0, got, own)
        dst[...] = cat(lo, hi).astype(BF)

    for cp in vec_copies:
        cp.wait()
    node_x.wait()
    node_in(VF.at[0], 0, 1)

    def vec_row(layer, row, node=False):
        ref = VN if node else VE
        return cat(ref[0, row, layer:layer + 1], ref[1, row, layer:layer + 1])

    def full1(ref, layer, k):
        return ref[layer, k].reshape(D, D)

    def gate(hidden):
        return 0.5 + 0.5 * jnp.tanh(0.5 * hidden)

    def second(act, ref, layer):
        return cat(dot(act, ref[layer, 0]), dot(act, ref[layer, 1]))

    def second_t(dout, ref, layer):
        return dot_cols(dout[:, :H], ref[layer, 0]) + dot_cols(dout[:, H:], ref[layer, 1])

    def add_message(dst, b, n, lat, msg):
        new = lat + msg.astype(F32)
        dst[0, edges(b, n)] = new[:, :H].reshape(n, NS, H).astype(BF)
        dst[1, edges(b, n)] = new[:, H:].reshape(n, NS, H).astype(BF)

    def layer_fwd(layer, src, dst):
        w_recv(4 * layer)
        PS[...] = (dot(VF[layer], full1(W1E, layer, 1)) + b1e[layer:layer + 1]).reshape(NN, NS, D)
        PR[...] = dot(VF[layer], full1(W1E, layer, 2)).reshape(NN, NS, D)
        if layer:
            start_all([grad_copy, node_g])
        else:
            w_recv(1)
            w_recv(2)
            lat_copy(2).start()
        c0, gam, bet = (vec_row(layer, r) for r in range(3))
        AG[...] = jnp.zeros_like(AG)

        def edge(b, carry):
            if not layer:
                lat_copy(b).wait()
                pl.when(b < 2)(lambda: lat_copy(b + 3).start())
                pl.when(b == 2)(w_copies[3].start)
                pl.when(b == 3)(w_copies[4].start)
                src[ot, edges(b, WIDE)] = CS[erows(b, WIDE), :H].reshape(WIDE, NS, H).astype(BF)
            for i in range(WIDE):
                GA[i * NS:(i + 1) * NS] = PS[snd[b * WIDE + i]] + PR[rcv[b * WIDE + i]]
            lat = cat(rows_of(src[0, edges(b, WIDE)]), rows_of(src[1, edges(b, WIDE)]))
            hidden = dot(lat.astype(BF), full1(W1E, layer, 0)) + GA[...]
            HS[erows(b, WIDE)] = hidden
            act = (hidden * gate(hidden)).astype(BF)
            out = second(act, W2E, layer) + c0
            cen = out - mean_cols(out)
            CS[erows(b, WIDE)] = cen
            normed, unused = norm_parts(cen)
            msg = (normed * gam + bet).astype(BF)
            AG[...] += dot_rows(KR[erows(b, WIDE)], msg)
            if not layer:
                add_message(dst, b, WIDE, lat, msg)
            return carry

        lax.fori_loop(0, NE // WIDE, edge, 0)
        if not layer:
            start_all(spills)
            w_recv(3)
        SF[layer] = AG[...].astype(BF)
        lat = VF[layer]
        hidden = dot(lat, full1(W1N, layer, 0)) + dot(SF[layer], full1(W1N, layer, 1)) + b1n[layer:layer + 1]
        HN[layer] = hidden
        act = (hidden * gate(hidden)).astype(BF)
        out = second(act, W2N, layer) + vec_row(layer, 0, True)
        cen = out - mean_cols(out)
        CN[layer] = cen
        normed, unused = norm_parts(cen)
        msg = (normed * vec_row(layer, 1, True) + vec_row(layer, 2, True)).astype(BF)
        VF[layer + 1] = (lat.astype(F32) + msg.astype(F32)).astype(BF)

    spills = [pltpu.make_async_copy(HS, spill.at[0], spsem.at[0]), pltpu.make_async_copy(CS, spill.at[1], spsem.at[1])]
    fills = [pltpu.make_async_copy(spill.at[0], HS, spsem.at[2]), pltpu.make_async_copy(spill.at[1], CS, spsem.at[3])]

    layer_fwd(0, E0, E1)
    select(KS, snd)
    wait_all(spills)
    layer_fwd(1, E1, None)
    grad_copy.wait()

    def grad_rows(b, carry):
        DE[ot, edges(b)] = R2[erows(b), H:].reshape(BE, NS, H).astype(BF)
        return carry

    lax.fori_loop(0, NB, grad_rows, 0)
    for peer in peers:
        pl.semaphore_signal(csem.at[0], inc=1, device_id=peer, device_id_type=MESH)
    node_g.wait()
    node_in(DN, 2, 3)

    def chunk(c):
        return 1 - c // 7, c % 7

    def g_copy(c, send, k, src, dst, peer):
        return pltpu.make_async_remote_copy(
            src_ref=src, dst_ref=dst, send_sem=gssem.at[c % 7, send], recv_sem=grsem.at[c % 7, k],
            device_id=peer, device_id_type=MESH)

    def core_copy(c):
        layer, j = chunk(c)
        return g_copy(c, 0, 0, G.at[layer, ot, j], R2.at[j * H:(j + 1) * H], partner)

    def landing(c):
        layer, j = chunk(c)
        if layer:
            return lambda lo, n: R2.at[7 * H + j * 192 + lo:7 * H + j * 192 + lo + n]
        return lambda lo, n: G.at[1, tp, j, lo:lo + n]

    half_p, half_q = cx * 64, 128 + cy * 64
    quarter_p, quarter_q = half_p + cy * 32, half_q + cx * 32

    def strip(c, start, n, final=False):
        layer, j = chunk(c)
        return G.at[layer, ot if final else tp, j, pl.ds(pl.multiple_of(start, 32), n)]

    def a_copies(c):
        land = landing(c)
        return [g_copy(c, 1, 1, strip(c, 64 - half_p, 64), land(0, 64), x_peer),
                g_copy(c, 2, 2, strip(c, 320 - half_q, 64), land(64, 64), y_peer)]

    def b_copies(c):
        land = landing(c)
        return [g_copy(c, 1, 3, strip(c, half_p + 32 - cy * 32, 32), land(128, 32), y_peer),
                g_copy(c, 2, 4, strip(c, half_q + 32 - cx * 32, 32), land(160, 32), x_peer)]

    def c_copies(c):
        ref_p, ref_q = strip(c, quarter_p, 32, True), strip(c, quarter_q, 32, True)
        return [g_copy(c, 1, 5, ref_p, ref_p, y_peer), g_copy(c, 2, 6, ref_q, ref_q, x_peer)]

    def d_copies(c):
        ref_p, ref_q = strip(c, half_p, 64, True), strip(c, half_q, 64, True)
        return [g_copy(c, 1, 7, ref_p, ref_p, x_peer), g_copy(c, 2, 8, ref_q, ref_q, y_peer)]

    def store_copies(c):
        layer, j = chunk(c)
        src = G.at[layer, ot, j]
        if j in (J_NW2, J_EW2):
            ref = o_nw2 if j == J_NW2 else o_ew2
            pairs = [(src.at[:, :H], ref.at[layer, :H]), (src.at[:, H:], ref.at[layer, H:])]
        elif j < J_EW2:
            pairs = [(src, o_nw1.at[layer, j - J_NW1])]
        else:
            pairs = [(src, o_ew1.at[layer, j - J_EW1])]
        return [pltpu.make_async_copy(a, b, osem.at[c % 7, k]) for k, (a, b) in enumerate(pairs)]

    def stage0(c):
        core_copy(c).start()

    def stage1(c):
        layer, j = chunk(c)
        core_copy(c).wait()
        G[layer, tp, j] += R2[j * H:(j + 1) * H]
        start_all(a_copies(c))

    def stage2(c):
        land = landing(c)
        wait_all(a_copies(c))
        for start, lo in ((half_p, 0), (half_q, 64)):
            ref = strip(c, start, 64)
            ref[...] += land(lo, 64)[...]
        start_all(b_copies(c))

    def stage3(c):
        land = landing(c)
        wait_all(b_copies(c))
        for start, lo in ((quarter_p, 128), (quarter_q, 160)):
            strip(c, start, 32, True)[...] = strip(c, start, 32)[...] + land(lo, 32)[...]
        start_all(c_copies(c))

    def stage4(c):
        wait_all(c_copies(c))
        start_all(d_copies(c))

    def stage5(c):
        wait_all(d_copies(c))
        if c >= 7:
            wait_all(store_copies(c - 7))
        start_all(store_copies(c))

    def run(stage, chunks):
        for c in chunks:
            stage(c)

    node1, edge1, node0, edge0 = (list(range(*ends)) for ends in ((0, 3), (3, 7), (7, 10), (10, 14)))

    plan = {
        1: [(stage2, node1, 1), (stage3, node1[:2], 3)],
        0: [(stage2, edge1, 0), (stage5, node1, 2), (stage3, edge1[:2], 3)],
    }

    def put_w2(layer, j, half, value, add):
        if add:
            G[layer, half, j, :, :H] += value[:H]
            G[layer, half, j, :, H:] += value[H:]
        else:
            G[layer, half, j, :, :H] = value[:H]
            G[layer, half, j, :, H:] = value[H:]

    def put_w1(layer, j, value, add=False):
        for half in range(2):
            if add:
                G[layer, half, j] += value[half * H:(half + 1) * H]
            else:
                G[layer, half, j] = value[half * H:(half + 1) * H]

    def mlp_bwd(d_msg, cen, hidden, gam, w2, layer, sm, j2, add):
        normed, inv_std = norm_parts(cen)
        sums = [sum_rows(d_msg * normed), sum_rows(d_msg)]
        d_normed = d_msg * gam
        d_out = inv_std * (d_normed - mean_cols(d_normed) - normed * mean_cols(d_normed * normed))
        sums = [sum_rows(d_out)] + sums
        d_out_bf = d_out.astype(BF)
        sig = gate(hidden)
        act = (hidden * sig).astype(BF)
        for half in range(2):
            put_w2(layer, j2, half, dot_rows(act, d_out_bf[:, half * H:(half + 1) * H]), add)
        d_hidden = second_t(d_out_bf, w2, layer) * (sig * (1.0 + hidden * (1.0 - sig)))
        sums = [sum_rows(d_hidden)] + sums
        for k in range(4):
            if add:
                SM[0, sm + k:sm + k + 1] += sums[k]
            else:
                SM[0, sm + k:sm + k + 1] = sums[k]
        return d_hidden.astype(BF)

    SM[...] = jnp.zeros_like(SM)

    def layer_bwd(layer, src):
        d_node = DN[...].astype(F32)
        d_hid = mlp_bwd(d_node, CN[layer], HN[layer], vec_row(layer, 1, True), W2N, layer, layer * 8, J_NW2, False)
        nodes, edge_w2, edge_w1 = (node1, edge1[:1], edge1[1:]) if layer else (node0, edge0[:1], edge0[1:])
        pl.semaphore_wait(csem.at[1 - layer], 3 if layer == 1 else 1)
        stage0(nodes[0])
        put_w1(layer, J_NW1, dot_rows(VF[layer], d_hid))
        stage0(nodes[1])
        stage1(nodes[0])
        put_w1(layer, J_NW1 + 1, dot_rows(SF[layer], d_hid))
        stage0(nodes[2])
        stage1(nodes[1])
        HN[layer] = d_node + dot_cols(d_hid, full1(W1N, layer, 0))
        PS[...] = dot_cols(d_hid, full1(W1N, layer, 1)).reshape(NN, NS, D)
        stage1(nodes[2])
        for j in (J_EW2, J_EW1):
            G[layer, :, j] = jnp.zeros((2, H, D), F32)
        AG[...] = jnp.zeros_like(AG)
        PR[...] = jnp.zeros_like(PR)
        gam, bet = vec_row(layer, 1), vec_row(layer, 2)
        if not layer:
            for cp in fills:
                cp.wait()

        def edge(b, carry):
            for i in range(BE):
                GA[i * NS:(i + 1) * NS] = PS[rcv[b * BE + i]]
            d_edge = cat(rows_of(DE[0, edges(b)]), rows_of(DE[1, edges(b)]))
            d_hid = mlp_bwd(d_edge + GA[:BE * NS], CS[erows(b)], HS[erows(b)], gam, W2E, layer, layer * 8 + 4, J_EW2, True)
            lat = cat(rows_of(src[0, edges(b)]), rows_of(src[1, edges(b)]))
            put_w1(layer, J_EW1, dot_rows(lat.astype(BF), d_hid), True)
            if layer:
                normed, unused = norm_parts(CS[erows(b)])
                add_message(E2, b, BE, lat, (normed * gam + bet).astype(BF))
            new = d_edge + dot_cols(d_hid, full1(W1E, layer, 0))
            DE[0, edges(b)] = new[:, :H].reshape(BE, NS, H).astype(BF)
            DE[1, edges(b)] = new[:, H:].reshape(BE, NS, H).astype(BF)
            AG[...] += dot_rows(KS[erows(b)], d_hid)
            PR[...] += dot_rows(KR[erows(b)], d_hid).reshape(NN, NS, D)
            for stage, chunks, first in plan[layer]:
                for i, c in enumerate(chunks):
                    pl.when(b == first + i)(functools.partial(stage, c))
            return carry

        lax.fori_loop(0, NB, edge, 0)
        if layer:
            for cp in fills:
                cp.start()
        run(stage0, edge_w2 + edge_w1[:1])
        run(stage3, (node1 if layer else edge1)[2:])
        run(stage4, node1[:2] if layer else edge1)
        d_ps, d_pr = AG[...].astype(BF), rows_of(PR[...]).astype(BF)
        put_w1(layer, J_EW1 + 1, dot_rows(VF[layer], d_ps))
        stage0(edge_w1[1])
        put_w1(layer, J_EW1 + 2, dot_rows(VF[layer], d_pr))
        stage0(edge_w1[2])
        DN[...] = (HN[layer] + dot_cols(d_ps, full1(W1E, layer, 1))
                   + dot_cols(d_pr, full1(W1E, layer, 2))).astype(BF)

    layer_bwd(1, E1)
    run(stage1, edge1)
    run(stage4, node1[2:])
    pl.semaphore_signal(csem.at[1], inc=1, device_id=partner, device_id_type=MESH)
    layer_bwd(0, E0)
    run(stage1, edge0)

    pl.semaphore_signal(csem.at[2], inc=1, device_id=partner, device_id_type=MESH)
    run(stage2, node0)
    for k, ref in ((0, VF.at[2]), (1, DN)):
        rows = ref[...].astype(F32)
        NST[2 * k] = jnp.where(tp == 0, rows[:, :H], rows[:, H:]).reshape(NN, NS, H).astype(BF)
        NF[2 * k] = jnp.where(tp == 0, rows[:, H:], rows[:, :H]).reshape(NN, NS, H)

    def out_stage(b, carry):
        HS[erows(b), :H] = rows_of(E2[ot, edges(b)])
        HS[erows(b), H:] = rows_of(DE[ot, edges(b)])
        return carry

    lax.fori_loop(0, NB, out_stage, 0)
    pl.semaphore_wait(csem.at[2], 1)
    small0 = rdma(SM.at[0], SM.at[1], 2)
    small0.start()
    node_o = [rdma(NF.at[0], NF.at[1], 4), rdma(NF.at[2], NF.at[3], 5)]
    for cp in node_o:
        cp.start()

    out_copy = rdma(HS, CS, 6)
    out_copy.start()
    stores = [
        (E2.at[tp], o_e.at[:, mine]), (DE.at[tp], o_de.at[:, mine]),
        (NST.at[0], o_n.at[:, mine]), (NST.at[2], o_dn.at[:, mine]),
    ]
    run(stage5, edge1)
    stores = [pltpu.make_async_copy(src, dst, lsem.at[i]) for i, (src, dst) in enumerate(stores)]
    for cp in stores:
        cp.start()
    for k, cp in enumerate(node_o):
        cp.wait()
        NST[2 * k + 1] = NF[2 * k + 1].astype(BF)

    def out_recv(b, carry):
        E1[0, edges(b)] = CS[erows(b), :H].reshape(BE, NS, H).astype(BF)
        E1[1, edges(b)] = CS[erows(b), H:].reshape(BE, NS, H).astype(BF)
        return carry

    run(stage3, node0)
    out_copy.wait()
    lax.fori_loop(0, NB, out_recv, 0)
    more = [
        (E1.at[0], o_e.at[:, theirs]), (E1.at[1], o_de.at[:, theirs]),
        (NST.at[1], o_n.at[:, theirs]), (NST.at[3], o_dn.at[:, theirs]),
    ]
    more = [pltpu.make_async_copy(src, dst, lsem.at[6 + i]) for i, (src, dst) in enumerate(more)]
    for cp in more:
        cp.start()
    small0.wait()
    SM[2] = SM[0] + SM[1]
    small1 = rdma(SM.at[2], SM.at[3], 3, x_peer)
    small1.start()
    run(stage2, edge0)
    run(stage4, node0)
    small1.wait()
    SM[4] = SM[2] + SM[3]
    small2 = rdma(SM.at[4], SM.at[5], 13, y_peer)
    small2.start()
    run(stage3, edge0)
    small2.wait()
    total = SM[4] + SM[5]
    for layer in range(2):
        for row, ref_b, ref_v in ((0, o_bn, o_vn), (4, o_be, o_ve)):
            at = layer * 8 + row
            ref_b[layer:layer + 1] = total[at:at + 1]
            for k in range(3):
                one = total[at + 1 + k:at + 2 + k]
                ref_v[k, layer:layer + 1] = jnp.where(tp == 0, one[:, :H], one[:, H:])
    run(stage4, edge0)
    run(stage5, node0 + edge0)
    for c in node0 + edge0:
        wait_all(store_copies(c))
    for cp in stores + more:
        cp.wait()


def compute(*args):
    any_spec = pl.BlockSpec(memory_space=pl.ANY)
    vm = pl.BlockSpec(memory_space=pltpu.VMEM)
    sm = pl.BlockSpec(memory_space=pltpu.SMEM)
    v = pltpu.VMEM
    lat = (NN, 2 * NS, H)
    edg = (NE, 2 * NS, H)
    outs = [(lat, BF), (edg, BF), (lat, BF), (edg, BF),
            ((2, 3, H, D), F32), ((2, D, H), F32), ((2, 2, H, D), F32), ((2, D, H), F32),
            ((2, D), F32), ((2, D), F32), ((3, 2, H), F32), ((3, 2, H), F32), ((2, NE * NS, D), F32)]
    dma = pltpu.SemaphoreType.DMA
    node = (ROWS, D)
    scratch = [
        v((2, 3, 2, H, D), BF), v((2, 2, D, H), BF), v((2, 2, 2, H, D), BF), v((2, 2, D, H), BF),
        *[v((2, 3, 2, H), F32)] * 2, *[v((NE * NS, ROWS), BF)] * 2, *[v((2, NE, NS, H), BF)] * 4,
        v((NE * NS, D), F32), v((NE * NS, D), F32), v((7 * (H + 192), D), F32), v((2, 2, 7, H, D), F32),
        v((NN, NS, D), F32), v((NN, NS, D), F32), v((WIDE * NS, D), F32), v(node, F32),
        v((4, NN, NS, H), BF), v((4, NN, NS, H), F32),
        v((3, *node), BF), v((2, *node), BF), v((2, *node), F32), v((2, *node), F32),
        v(node, BF), v((6, 16, D), F32),
        dma((12,)), dma((19,)), dma((19,)), pltpu.SemaphoreType.REGULAR((3,)), dma((4,)),
        dma((7, 3)), dma((7, 9)), dma((7, 2)),
    ]
    return pl.pallas_call(
        body,
        out_shape=[jax.ShapeDtypeStruct(*o) for o in outs],
        in_specs=[any_spec] * 8 + [vm] * 4 + [sm] * 2,
        out_specs=[any_spec] * 8 + [vm] * 4 + [any_spec],
        scratch_shapes=scratch,
        compiler_params=pltpu.CompilerParams(
            collective_id=0, has_side_effects=True, vmem_limit_bytes=67043328),
    )(*args)


def mover(*refs):
    n = (len(refs) - 2) // 3
    pieces = []
    for src, dst, buf in zip(refs[:n], refs[n:2 * n], refs[2 * n:]):
        step = -(-src.shape[0] // (4 if src.size > 1 << 18 else 1))
        for lo in range(0, src.shape[0], step):
            at = pl.ds(lo, min(step, src.shape[0] - lo))
            k = len(pieces)
            pieces.append((pltpu.make_async_copy(src.at[at], buf.at[at], refs[-2].at[k]),
                           pltpu.make_async_copy(buf.at[at], dst.at[at], refs[-1].at[k])))
    for get, unused in pieces:
        get.start()
    for get, put in pieces:
        get.wait()
        put.start()
    for unused, put in pieces:
        put.wait()


def move(arrays):
    any_spec = pl.BlockSpec(memory_space=pl.ANY)
    shapes = [jax.ShapeDtypeStruct(x.shape, x.dtype) for x in arrays]
    return pl.pallas_call(
        mover, out_shape=shapes, in_specs=[any_spec] * len(arrays), out_specs=[any_spec] * len(arrays),
        scratch_shapes=[pltpu.VMEM(x.shape, x.dtype) for x in arrays] + [pltpu.SemaphoreType.DMA((24,))] * 2,
        compiler_params=pltpu.CompilerParams(vmem_limit_bytes=67043328))(*arrays)


def solution(mesh):
    lat_spec = P('dp', None, 'tp')
    first_spec = P(None, None, 'tp', None)
    col_spec = P(None, None, 'tp')
    param_specs = (first_spec, P(), col_spec, col_spec, first_spec, P(), col_spec, col_spec)
    in_specs = (lat_spec, lat_spec, P(), P(), lat_spec, lat_spec) + param_specs
    out_specs = (lat_spec, lat_spec, lat_spec, lat_spec) + param_specs

    def local_step(node_lat, edge_lat, senders, receivers, grad_node, grad_edge, edge_w1, edge_b1, edge_w2, edge_vec, node_w1, node_b1, node_w2, node_vec):
        def swap(x):
            return jnp.transpose(x, (1, 0, 2))

        outs = compute(
            swap(node_lat), swap(edge_lat), swap(grad_node), swap(grad_edge), edge_w1, edge_w2, node_w1, node_w2,
            edge_b1, node_b1, swap(edge_vec), swap(node_vec), senders, receivers)
        outs = move(outs[:12])
        o_ew1, o_ew2, o_nw1, o_nw2, o_be, o_bn, o_ve, o_vn = outs[4:]
        return tuple(swap(x) for x in outs[:4]) + (o_ew1, o_be, o_ew2, swap(o_ve), o_nw1, o_bn, o_nw2, swap(o_vn))

    return jax.shard_map(local_step, mesh=mesh, in_specs=in_specs, out_specs=out_specs, check_vma=False)
```
